32 devices in a mesh: len: 2 (over x), wid: 4 (over z), dep: 4 (over y, core).
Axes of the slice: x: 2, y: 2, z: 4, core: 2. Of those that a mesh axis runs over, the one named last changes fastest.
Arguments:
- coords: float32 [3, 32768], P(None, ('len', 'wid', 'dep')), may hold values from -3 to 3
- velocity: float32 [3, 32768], P(None, ('len', 'wid', 'dep')), may hold values from -6 to 6
- node_mass: float32 [32768], P(('len', 'wid', 'dep')), may hold values from 0.5 to 2
- corner_nodes: int32 [4, 32768], P(None, ('len', 'wid', 'dep')), may hold values from 0 to 1151, as said below
- shape_grad: float32 [8, 32768], P(None, ('len', 'wid', 'dep')), may hold values from -5 to 5
- frame_angles: float32 [2, 32768], P(None, ('len', 'wid', 'dep')), may hold values from -3.140625 to 3.140625
- volume: float32 [32768], P(('len', 'wid', 'dep')), may hold values from 0.5 to 2
- stress: float32 [3, 32768], P(None, ('len', 'wid', 'dep')), may hold values from -5 to 5
- send_nodes: int32 [32, 16, 256], P(('len', 'wid', 'dep')), may hold values from 0 to 1023
- tile_count: int32 [32], P(('len', 'wid', 'dep')), may hold values from 1 to 4, as said below
- tile_nodes: int32 [128, 128], P(('len', 'wid', 'dep')), may hold values from 0 to 4095
- tile_facets: int32 [4, 128, 128], P(None, ('len', 'wid', 'dep')), may hold values from 0 to 4095
- pair_mask: int32 [128, 128, 128], P(('len', 'wid', 'dep')), may hold values 0 or 1
Outputs:
- coords_out: float32 [3, 32768], P(None, ('len', 'wid', 'dep'))
- velocity_out: float32 [3, 32768], P(None, ('len', 'wid', 'dep'))
- stress_out: float32 [3, 32768], P(None, ('len', 'wid', 'dep'))
The draws below stay inside these ranges and needn't reach their ends.
Inputs may be any that keep to these rules, and one draw needn't show every extreme that they name: `corner_nodes`: for the element at device-local position i (i = e mod 1024), every entry lies from (i // 128) * 128 to (i // 128) * 128 + 2 * 128 - 1. An entry j below 1024 names the element device's own node j; an entry 1024 + i names node i of the next device in the order len, wid, dep, the last device's next being the first. `send_nodes`: entry [p, g, k] is a node of device p, by its local number, sent to device g of p's slab; nodes may repeat. `tile_count`: some device has 4 live tiles in every draw; a device's tiles at and past its count are not used. `tile_nodes`: slot g * 256 + k of the tile's device is slot k of what device g of its slab sends it. `tile_facets`: slots as for tile_nodes, one for each of a facet's four corners.
All inputs are finite; a program needn't handle non-finite values. No bound on the sum of `pair_mask` on one device may be relied on, other than what follows from the above.
Results may differ from the reference program's by a relative error of at most 0.0003.
Values sent between devices are 32-bit elements; how exact they have to be, the bound alone decides.
A program may use at most 64 MiB of HBM per device.

```python
import math
import jax
import jax.numpy as jnp
from jax import lax

ELEM_DEV = 1024
NODE_DEV = 1024
RIM = 128
SEND_CAP = 256
TILE_CAP = 4
TILE_NODE = 128
TILE_FACET = 128
STEPS = 2
GROUP = 16
ELEMS = 32768
NODES = 32768
TILES = 128
N_LEN = 2
N_WID = 4
N_DEP = 4
DEVICES = 32


def draw_tile_count(key, part):
    key_heavy = jax.random.fold_in(key, 11)
    key_light = jax.random.fold_in(key, 12)
    key_chosen = jax.random.fold_in(key, 13)
    is_heavy = jax.random.randint(key_heavy, (DEVICES,), 0, 8) == 0
    light_count = jax.random.randint(key_light, (DEVICES,), 1, max(TILE_CAP // 4, 1) + 1)
    counts = jnp.where(is_heavy, TILE_CAP, light_count)
    chosen = jax.random.randint(key_chosen, (), 0, DEVICES)
    return jnp.where(jnp.arange(DEVICES) == chosen, TILE_CAP, counts).astype(jnp.int32)


def draw_corner_nodes(key, part):
    key_offset = jax.random.fold_in(key, 21)
    position = jnp.arange(ELEMS, dtype=jnp.int32) % ELEM_DEV
    block_start = position // RIM * RIM
    offset = jax.random.randint(key_offset, (4, ELEMS), 0, 2 * RIM)
    return (block_start[None, :] + offset).astype(jnp.int32)


def set_ends(drawn, key, least, high):
    longest = drawn.shape.index(max(drawn.shape))
    spots = []
    for shift in (0, 1):
        where = [jax.random.randint(jax.random.fold_in(key, axis), (), 0, length) for axis, length in enumerate(drawn.shape)]
        where[longest] = (where[longest] + shift) % drawn.shape[longest]
        spots.append(tuple(where))
    return drawn.at[spots[0]].set(least).at[spots[1]].set(high)


def steps_of(stream_key, extent, cuts, low, largest):
    level = 1.0
    for dim, shards_of in cuts:
        steps = jax.random.uniform(jax.random.fold_in(jax.random.fold_in(stream_key, 6), dim), (shards_of,), jnp.float32, low / len(cuts), largest / len(cuts))
        level = level * jnp.repeat(jnp.exp(steps), extent[dim] // shards_of).reshape((-1,) + (1,) * (len(extent) - 1 - dim))
    return level


def bell_draw(stream_key, shape, deviation, bound, shards=(), kind=jnp.bfloat16):
    values = deviation * jax.random.normal(stream_key, shape, jnp.float32)
    if shards:
        values = values * steps_of(stream_key, shape, shards, -0.22, 0.18)
    return jnp.clip(values, -bound, bound).astype(kind)


def setup_inputs(seed: int = 0) -> dict:
    splits = jax.random.split(jax.random.key(seed), 14)
    coords = bell_draw(splits[0], (3, NODES), 0.5, 3.0, ((1, 32),), jnp.float32)
    velocity = bell_draw(splits[1], (3, NODES), 1.0, 6.0, ((1, 32),), jnp.float32)
    node_mass = jnp.clip(jnp.exp(math.log(2.0) - 1.3862944 * jax.random.uniform(splits[2], (NODES,), jnp.float32) ** steps_of(splits[2], (NODES,), ((0, 32),), -0.2, 0.2)), 0.5, 2.0)
    corner_nodes = draw_corner_nodes(jax.random.fold_in(splits[13], 71), 0)
    shape_grad = bell_draw(splits[4], (8, ELEMS), 1.0, 5.0, ((1, 32),), jnp.float32)
    frame_angles = jnp.clip(jax.random.uniform(splits[5], (2, ELEMS), jnp.float32, -3.140625, 3.140625), -3.140625, 3.140625)
    volume = jnp.clip(jnp.exp(math.log(2.0) - 1.3862944 * jax.random.uniform(splits[6], (ELEMS,), jnp.float32) ** steps_of(splits[6], (ELEMS,), ((0, 32),), -0.2, 0.2)), 0.5, 2.0)
    stress = bell_draw(splits[7], (3, ELEMS), 1.0, 5.0, ((1, 32),), jnp.float32)
    send_nodes = set_ends(jax.random.randint(splits[8], (DEVICES, GROUP, SEND_CAP), 0, NODE_DEV), jax.random.fold_in(splits[8], 1), 0, NODE_DEV - 1).astype(jnp.int32)
    tile_count = draw_tile_count(jax.random.fold_in(splits[13], 71), 0)
    tile_nodes = set_ends(jax.random.randint(splits[10], (TILES, TILE_NODE), 0, GROUP * SEND_CAP), jax.random.fold_in(splits[10], 1), 0, (GROUP * SEND_CAP) - 1).astype(jnp.int32)
    tile_facets = set_ends(jax.random.randint(splits[11], (4, TILES, TILE_FACET), 0, GROUP * SEND_CAP), jax.random.fold_in(splits[11], 1), 0, (GROUP * SEND_CAP) - 1).astype(jnp.int32)
    pair_mask = set_ends((jax.random.randint(splits[12], (TILES, TILE_NODE, TILE_FACET), 0, 2) < 1).astype(jnp.int32), jax.random.fold_in(splits[12], 1), 0, 1)
    return {"coords": coords, "velocity": velocity, "node_mass": node_mass, "corner_nodes": corner_nodes, "shape_grad": shape_grad, "frame_angles": frame_angles, "volume": volume, "stress": stress, "send_nodes": send_nodes, "tile_count": tile_count, "tile_nodes": tile_nodes, "tile_facets": tile_facets, "pair_mask": pair_mask}


TIME_STEP = 0.1
YOUNG_MOD = 1.0
POISSON = 0.3
HOURGLASS = 0.1
RADIUS_SQ = 1.0
STIFFNESS = 0.1
DAMPING = 0.05


def frame_vectors(frame_angles):
    polar_angle = frame_angles[0]
    azimuth = frame_angles[1]
    axis_one = jnp.stack([jnp.cos(polar_angle) * jnp.cos(azimuth), jnp.cos(polar_angle) * jnp.sin(azimuth), -jnp.sin(polar_angle)])
    axis_two = jnp.stack([-jnp.sin(azimuth), jnp.cos(azimuth), jnp.zeros_like(azimuth)])
    return axis_one, axis_two


def element_forces(corner_vel, shape_grad, axis_one, axis_two, volume, stress):
    grad_x = shape_grad[:4]
    grad_y = shape_grad[4:]
    along_one = jnp.sum(axis_one[:, None, :] * corner_vel, axis=0)
    along_two = jnp.sum(axis_two[:, None, :] * corner_vel, axis=0)
    rate_xx = jnp.sum(grad_x * along_one, axis=0)
    rate_yy = jnp.sum(grad_y * along_two, axis=0)
    rate_xy = jnp.sum(grad_y * along_one + grad_x * along_two, axis=0)
    factor = TIME_STEP * YOUNG_MOD / (1.0 - POISSON * POISSON)
    sigma_xx = stress[0] + factor * (rate_xx + POISSON * rate_yy)
    sigma_yy = stress[1] + factor * (POISSON * rate_xx + rate_yy)
    sigma_xy = stress[2] + factor * 0.5 * (1.0 - POISSON) * rate_xy
    hourglass_mode = jnp.array([1.0, -1.0, 1.0, -1.0], jnp.float32)[:, None]
    hourglass_rate = jnp.sum(hourglass_mode[None] * corner_vel, axis=1)
    force_one = -volume * (grad_x * sigma_xx + grad_y * sigma_xy)
    force_two = -volume * (grad_y * sigma_yy + grad_x * sigma_xy)
    corner_force = axis_one[:, None] * force_one[None] + axis_two[:, None] * force_two[None] - HOURGLASS * volume * hourglass_mode[None] * hourglass_rate[:, None]
    return corner_force, jnp.stack([sigma_xx, sigma_yy, sigma_xy])


def tile_forces(node_coordinates, node_velocities, corner_pos, corner_vel, pair_bits, live_row):
    facet_centroid = 0.25 * jnp.sum(corner_pos, axis=1)
    centroid_velocity = 0.25 * jnp.sum(corner_vel, axis=1)
    inner_product = jnp.einsum("ywq,ywk->wqk", node_coordinates, facet_centroid, precision=lax.Precision.HIGHEST)
    distance = jnp.sum(node_coordinates * node_coordinates, axis=0)[:, :, None] + jnp.sum(facet_centroid * facet_centroid, axis=0)[:, None, :] - 2.0 * inner_product
    corner_weight = pair_bits.astype(jnp.float32) * live_row[:, None, None] * jnp.maximum(RADIUS_SQ - distance, 0.0)
    row_sum = jnp.sum(corner_weight, axis=2)
    col_sum = jnp.sum(corner_weight, axis=1)
    gathered_positions = jnp.einsum("yml,mjl->ymj", facet_centroid, corner_weight, precision=lax.Precision.HIGHEST)
    gathered_velocities = jnp.einsum("yml,mjl->ymj", centroid_velocity, corner_weight, precision=lax.Precision.HIGHEST)
    node_force = STIFFNESS * (row_sum * node_coordinates - gathered_positions) - DAMPING * (row_sum * node_velocities - gathered_velocities)
    outgoing_positions = jnp.einsum("ewo,woj->ewj", node_coordinates, corner_weight, precision=lax.Precision.HIGHEST)
    outgoing_velocities = jnp.einsum("ewo,woj->ewj", node_velocities, corner_weight, precision=lax.Precision.HIGHEST)
    facet_force = STIFFNESS * (outgoing_positions - col_sum * facet_centroid) - DAMPING * (outgoing_velocities - col_sum * centroid_velocity)
    return node_force, -0.25 * facet_force


def reference(coords, velocity, node_mass, corner_nodes, shape_grad, frame_angles, volume, stress, send_nodes, tile_count, tile_nodes, tile_facets, pair_mask):
    group_size = N_WID * N_DEP
    owners = jnp.arange(ELEMS, dtype=jnp.int32) // ELEM_DEV
    node_of = ((owners[None, :] * NODE_DEV + corner_nodes) % NODES).astype(jnp.int32)
    axis_one, axis_two = frame_vectors(frame_angles)
    sources = jnp.arange(DEVICES, dtype=jnp.int32)
    global_send = (sources[:, None, None] * NODE_DEV + send_nodes).astype(jnp.int32)
    by_source = global_send.reshape(N_LEN, group_size, group_size, SEND_CAP)
    slot_node = jnp.transpose(by_source, (0, 2, 1, 3)).reshape(DEVICES, group_size * SEND_CAP)
    nodes_three = tile_nodes.reshape(DEVICES, TILE_CAP, TILE_NODE)
    node_ids = slot_node[sources[:, None, None], nodes_three]
    facets_four = jnp.transpose(tile_facets.reshape(4, DEVICES, TILE_CAP, TILE_FACET), (1, 0, 2, 3))
    facet_ids = slot_node[sources[:, None, None, None], facets_four]
    live_tiles = (jnp.arange(TILE_CAP, dtype=jnp.int32)[None, :] < tile_count[:, None]).astype(jnp.float32)
    pair_bits = pair_mask.reshape(DEVICES, TILE_CAP, TILE_NODE, TILE_FACET)
    for repeat in range(STEPS):
        corner_force, stress = element_forces(velocity[:, node_of], shape_grad, axis_one, axis_two, volume, stress)
        internal = jnp.zeros((3, NODES), jnp.float32).at[:, node_of].add(corner_force)

        def per_device(pieces, coords=coords, velocity=velocity):
            ids_node, ids_facet, bit_rows, live_row = pieces
            return tile_forces(coords[:, ids_node], velocity[:, ids_node], coords[:, ids_facet], velocity[:, ids_facet], bit_rows, live_row)

        node_force, facet_share = lax.map(per_device, (node_ids, facet_ids, pair_bits, live_tiles))
        node_force = jnp.transpose(node_force, (1, 0, 2, 3))
        facet_share = jnp.transpose(facet_share, (1, 0, 2, 3))
        contact = jnp.zeros((3, NODES), jnp.float32).at[:, node_ids].add(node_force)
        for corner in range(4):
            contact = contact.at[:, facet_ids[:, corner]].add(facet_share)
        velocity = velocity + TIME_STEP * (internal + contact) / node_mass
        coords = coords + TIME_STEP * velocity
    return coords, velocity, stress
```

```python
import functools

import jax
import jax.numpy as jnp
from jax import lax
from jax.experimental import pallas as pl
from jax.experimental.pallas import tpu as pltpu
from jax.sharding import PartitionSpec as P

STEPS = 2
TIME_STEP = 0.1
YOUNG_MOD = 1.0
POISSON = 0.3
HOURGLASS = 0.1
RADIUS_SQ = 1.0
STIFFNESS = 0.1
DAMPING = 0.05

LANES = 128
MESH = pl.DeviceIdType.MESH
F32 = jnp.float32
BF16 = jnp.bfloat16


def two_parts(values):
    first = values.astype(BF16)
    return first, (values - first.astype(F32)).astype(BF16)


def lane_take(table, low):
    return jnp.take_along_axis(table, low, axis=1, mode="promise_in_bounds")


def nt_dot(left, right):
    return lax.dot_general(left, right, (((1,), (1,)), ((), ())), preferred_element_type=F32)


def nn_dot(left, right):
    return lax.dot_general(left, right, (((1,), (0,)), ((), ())), preferred_element_type=F32)


def kernel(
    sizes,
    coords_hbm, velocity_hbm, mass_hbm, corner_hbm, grad_hbm, angles_hbm, volume_hbm, stress_hbm,
    send_hbm, nodes_hbm, facets_hbm, mask_hbm, count_in,
    coords_out, velocity_out, stress_out,
    coords_in, velocity_in, mass_in, corner_in, grad_in, angles_in, volume_in, stress_in,
    send_in, nodes_in, facets_in, mask_in, in_sem,
    pos, vel, corner, grad, stress, angle, slot_ids, tile_ids, win_hot, tile_hot, node_hot,
    win_rows, force_rows, tile_lhs, node_lhs,
    send_buf, recv_buf, again_buf, fresh_buf, back_buf, answer_buf,
    first_buf, last_buf, ghost_recv, last_recv,
    corner_prev, grad_prev, angles_prev, volume_prev, stress_prev,
    out_send_sem, out_recv_sem, back_send_sem, back_recv_sem, edge_send_sem, edge_recv_sem,
    prev_send_sem, prev_recv_sem,
):
    n_len, n_wid, n_dep = sizes
    group = n_wid * n_dep
    devices = n_len * group
    rows = coords_in.shape[1] // LANES
    halves = send_in.shape[2] // LANES
    tiles = nodes_in.shape[0]
    my_len = lax.axis_index("len")
    my_wid = lax.axis_index("wid")
    my_dep = lax.axis_index("dep")
    my_place = my_wid * n_dep + my_dep
    my_id = my_len * group + my_place

    def by_id(p):
        return (p // group, (p % group) // n_dep, p % n_dep)

    upper = (2 * my_wid) // n_wid
    shifts = sorted(range(1, n_dep), key=lambda d: -min(d, n_dep - d))
    peers = []
    for r in range(n_wid):
        across = r + (1 - upper) * (n_wid - 1 - 2 * r)
        for shift in shifts:
            peers.append((across, lax.rem(my_dep + shift, n_dep)))
        if r < n_wid - 1:
            up = r + (r - my_wid + n_wid) // n_wid
            down = n_wid - 1 - r - (my_wid - (n_wid - 1 - r) + n_wid) // n_wid
            peers.append((upper * up + (1 - upper) * down, my_dep))
    places = [wid * n_dep + dep for wid, dep in peers]
    count = group - 1
    arrival = [my_place] + places[::-1]

    before = by_id(lax.rem(my_id + devices - 1, devices))
    after = by_id(lax.rem(my_id + 1, devices))

    loads = [
        pltpu.make_async_copy(src, dst, in_sem.at[n])
        for n, (src, dst) in enumerate((
            (send_hbm, send_in), (velocity_hbm, velocity_in), (coords_hbm, coords_in),
            (corner_hbm, corner_in), (stress_hbm, stress_in), (grad_hbm, grad_in),
            (angles_hbm, angles_in), (mass_hbm, mass_in), (volume_hbm, volume_in),
            (nodes_hbm, nodes_in), (facets_hbm, facets_in), (mask_hbm, mask_in),
        ))
    ]
    for load in loads[:3]:
        load.start()
    barrier = pltpu.get_barrier_semaphore()
    for wid, dep in peers:
        pl.semaphore_signal(barrier, inc=1, device_id=(my_len, wid, dep), device_id_type=MESH)
    pl.semaphore_signal(barrier, inc=1, device_id=before, device_id_type=MESH)
    pl.semaphore_signal(barrier, inc=1, device_id=after, device_id_type=MESH)
    for load in loads[3:]:
        load.start()
    for load in loads[:3]:
        load.wait()
    for i in range(rows):
        cols = pl.ds(i * LANES, LANES)
        pos[pl.ds(i, 3, stride=rows), :] = coords_in[:, cols]
        for k in range(3):
            vel[pl.ds(k * 2 * rows + i, 1), :] = velocity_in[pl.ds(k, 1), cols]

    def velocity_rows(k):
        return vel[pl.ds(k * 2 * rows, rows), :]

    def fill_edges(step):
        for k in range(3):
            first_buf[step - 1, pl.ds(k, 1), :] = vel[pl.ds(k * 2 * rows, 1), :]
            last_buf[step - 1, pl.ds(k, 1), :] = vel[pl.ds(k * 2 * rows + rows - 1, 1), :]

    def fill_slots(step):
        tables = [velocity_rows(k) for k in range(3)]
        if step == 0:
            tables += [pos[pl.ds(k * rows, rows), :] for k in range(3)]
        for half in range(halves):
            ids = send_in[0, :, pl.ds(half * LANES, LANES)]
            low, high = ids & (LANES - 1), ids >> 7
            if step == 0:
                slot_ids[:, half, :] = ids
            for c, table in enumerate(tables):
                found = jnp.zeros(ids.shape, F32)
                for h in range(rows):
                    row = jnp.broadcast_to(table[h : h + 1], ids.shape)
                    found = jnp.where(high == h, lane_take(row, low), found)
                if step == 0:
                    send_buf[:, c * halves + half, :] = found
                else:
                    again_buf[step - 1, :, c * halves + half, :] = found

    def remote(src, dst, send_sem, recv_sem, target):
        return pltpu.make_async_remote_copy(
            src_ref=src, dst_ref=dst, send_sem=send_sem, recv_sem=recv_sem,
            device_id=target, device_id_type=MESH,
        )

    final = pl.ds((rows - 1) * LANES, LANES)

    def edge_copies(step):
        if step == 0:
            first, last = velocity_in.at[:, pl.ds(0, LANES)], velocity_in.at[:, final]
        else:
            first, last = first_buf.at[step - 1], last_buf.at[step - 1]
        return (
            remote(first, ghost_recv.at[step], edge_send_sem.at[step, 0], edge_recv_sem.at[step, 0], before),
            remote(last, last_recv.at[step], edge_send_sem.at[step, 1], edge_recv_sem.at[step, 1], after),
        )

    def prev_copies():
        pairs = (
            (corner_in.at[:, final], corner_prev), (grad_in.at[:, final], grad_prev),
            (angles_in.at[:, final], angles_prev), (stress_in.at[:, final], stress_prev),
            (volume_in.at[pl.ds(rows - 1, 1), :], volume_prev),
        )
        return [
            remote(src, dst, prev_send_sem.at[n], prev_recv_sem.at[n], after)
            for n, (src, dst) in enumerate(pairs)
        ]

    def group_copy(step, j, back):
        wid, dep = peers[j]
        place = places[j]
        if back:
            src, dst, ss, rs = back_buf.at[step], answer_buf.at[step], back_send_sem, back_recv_sem
        elif step == 0:
            src, dst, ss, rs = send_buf, recv_buf, out_send_sem, out_recv_sem
        else:
            src, dst, ss, rs = again_buf.at[step - 1], fresh_buf.at[step - 1], out_send_sem, out_recv_sem
        return remote(
            src.at[place], dst.at[my_place], ss.at[step, j], rs.at[step, my_place], (my_len, wid, dep)
        )

    def group_arrival(step, j, back):
        wid, dep = peers[j]
        place = places[j]
        if back:
            src, dst, ss, rs = back_buf.at[step], answer_buf.at[step], back_send_sem, back_recv_sem
        elif step == 0:
            src, dst, ss, rs = send_buf, recv_buf, out_send_sem, out_recv_sem
        else:
            src, dst, ss, rs = again_buf.at[step - 1], fresh_buf.at[step - 1], out_send_sem, out_recv_sem
        return remote(
            src.at[place], dst.at[place], ss.at[step, j], rs.at[step, place], (my_len, wid, dep)
        )

    fill_slots(0)
    pl.semaphore_wait(barrier, group + 1)

    sub = lax.broadcasted_iota(jnp.int32, (LANES, LANES), 0)
    for step in range(STEPS):
        for j in range(count):
            group_copy(step, j, False).start()
        for copy in edge_copies(step):
            copy.start()

        if step == 0:
            for load in loads[3:]:
                load.wait()
            for copy in prev_copies():
                copy.start()
            for i in range(rows):
                cols = pl.ds(i * LANES, LANES)
                stress[pl.ds(i, 3, stride=rows), :] = stress_in[:, cols]
                corner[pl.ds(i, 4, stride=rows), :] = corner_in[:, cols]
                grad[pl.ds(i, 8, stride=rows), :] = grad_in[:, cols]
                angle[pl.ds(i, 2, stride=rows), :] = angles_in[:, cols]
            tile_ids[...] = jnp.zeros_like(tile_ids)
            tile_ids[pl.ds(0, tiles), :] = nodes_in[...]
            for a in range(4):
                tile_ids[pl.ds((a + 1) * tiles, tiles), :] = facets_in[a]
            first_row = lax.broadcasted_iota(jnp.int32, (rows, LANES), 0) * LANES
            corner_low, corner_far = [], []
            for a in range(4):
                local = corner[pl.ds(a * rows, rows), :] - first_row
                corner_low.append(local & (LANES - 1))
                corner_far.append(local >= LANES)
                for i in range(rows):
                    hot = (sub == corner_low[a][i : i + 1]).astype(F32).astype(BF16)
                    win_hot[i, :, pl.ds(a * LANES, LANES)] = hot
            polar, azim = angle[pl.ds(0, rows), :], angle[pl.ds(rows, rows), :]

            def frame(polar, azim):
                cos_p, sin_p, cos_a, sin_a = jnp.cos(polar), jnp.sin(polar), jnp.cos(azim), jnp.sin(azim)
                return (cos_p * cos_a, cos_p * sin_a, -sin_p), (-sin_a, cos_a)

            volume = volume_in[...]
            mass = mass_in[...]
            gx = [grad[pl.ds(a * rows, rows), :] for a in range(4)]
            gy = [grad[pl.ds((4 + a) * rows, rows), :] for a in range(4)]
            own = (frame(polar, azim), volume, gx, gy, corner_low, corner_far)
            for b in range(5 * tiles):
                low = tile_ids[pl.ds(b, 1), :] & (LANES - 1)
                tile_hot[:, pl.ds(b * LANES, LANES)] = (sub == low).astype(F32).astype(BF16)
            for n, g in enumerate(arrival):
                for half in range(halves):
                    low = slot_ids[g, pl.ds(half, 1), :] & (LANES - 1)
                    node_hot[:, pl.ds((n * halves + half) * LANES, LANES)] = (
                        (sub == low).astype(F32).astype(BF16)
                    )
            ids = tile_ids[...]
            ids_low, ids_high = ids & (LANES - 1), ids >> 7

        mine = send_buf if step == 0 else again_buf.at[step - 1]
        landed = recv_buf if step == 0 else fresh_buf.at[step - 1]
        found = [jnp.zeros(ids.shape, F32) for c in range(6 if step == 0 else 3)]
        for n, g in enumerate(arrival):
            if n:
                group_arrival(step, count - n, False).wait_recv()
            source = landed if n else mine
            for half in range(halves):
                match = ids_high == g * halves + half
                for c in range(len(found)):
                    row = jnp.broadcast_to(source[g, pl.ds(c * halves + half, 1), :], ids.shape)
                    found[c] = jnp.where(match, lane_take(row, ids_low), found[c])
        if step == 0:
            slot_pos = found[3:]
        else:
            slot_pos = [slot_pos[k] + TIME_STEP * found[k] for k in range(3)]
        state = slot_pos + found[:3]
        centre = [
            0.25 * sum(s[(a + 1) * tiles : (a + 2) * tiles] for a in range(4)) for s in state
        ]
        nodes = [s[:tiles] for s in state]
        node_mix = [STIFFNESS * nodes[k] - DAMPING * nodes[3 + k] for k in range(3)]
        facet_mix = [STIFFNESS * centre[k] - DAMPING * centre[3 + k] for k in range(3)]
        lead = jnp.concatenate(nodes[:3] + [jnp.zeros((16 - 3 * tiles % 16, LANES), F32)], axis=0)
        columns = jnp.transpose(lead)
        ones = jnp.ones((1, LANES), F32)
        blank = jnp.zeros((4, LANES), F32)
        node_force = [[None] * tiles for k in range(3)]
        facet_force = [[None] * tiles for k in range(3)]
        for t in range(tiles):
            live = jnp.where(t < count_in[0], 1.0, 0.0)
            dist = jnp.zeros((LANES, LANES), F32)
            for k in range(3):
                gap = columns[:, k * tiles + t : k * tiles + t + 1] - centre[k][t : t + 1]
                dist += gap * gap
            weight = mask_in[t].astype(F32) * (live * jnp.maximum(RADIUS_SQ - dist, 0.0))
            w1, w2 = two_parts(weight)
            a1, a2 = two_parts(jnp.concatenate([m[t : t + 1] for m in node_mix] + [ones, blank], axis=0))
            b1, b2 = two_parts(jnp.concatenate([m[t : t + 1] for m in facet_mix] + [ones, blank], axis=0))
            left_a = jnp.concatenate([a1, a2], axis=0)
            left_b = jnp.concatenate([b1, b2], axis=0)
            to_facet = nn_dot(
                jnp.concatenate([left_a, left_a], axis=1), jnp.concatenate([w1, w2], axis=0)
            )
            to_node = nt_dot(
                jnp.concatenate([left_b, left_b], axis=1), jnp.concatenate([w1, w2], axis=1)
            )
            to_facet = to_facet[:8] + to_facet[8:]
            to_node = to_node[:8] + to_node[8:]
            for k in range(3):
                node_force[k][t] = node_mix[k][t : t + 1] * to_node[3:4] - to_node[k : k + 1]
                facet_force[k][t] = -0.25 * (
                    to_facet[k : k + 1] - to_facet[3:4] * facet_mix[k][t : t + 1]
                )
        spans = halves * group
        high_iota = lax.broadcasted_iota(jnp.int32, (spans, LANES), 0)
        for b in range(5 * tiles):
            high = ids_high[b : b + 1]
            match = high_iota == (high % halves) * group + high // halves
            for k in range(3):
                row = node_force[k][b] if b < tiles else facet_force[k][b % tiles]
                chosen = jnp.where(match, jnp.broadcast_to(row, match.shape), 0.0)
                p1, p2 = two_parts(chosen)
                cols = pl.ds(b * LANES, LANES)
                tile_lhs[pl.ds(k * spans, spans), cols] = p1
                tile_lhs[pl.ds((3 + k) * spans, spans), cols] = p2
        slots = nt_dot(tile_lhs[...], tile_hot[...])
        slots = slots[: 3 * spans] + slots[3 * spans :]
        for r in range(3 * halves):
            back_buf[step, :, r, :] = slots[r * group : (r + 1) * group]
        for j in range(count):
            group_copy(step, j, True).start()

        if step == 0:
            for copy in prev_copies():
                copy.wait_recv()

            def whole(row):
                return jnp.broadcast_to(row, (8, LANES))

            prev_low, prev_far = [], []
            for a in range(4):
                local = corner_prev[pl.ds(a, 1), :] - (rows - 1) * LANES
                low = local & (LANES - 1)
                win_hot[rows, :, pl.ds(a * LANES, LANES)] = (sub == low).astype(F32).astype(BF16)
                prev_low.append(whole(low))
                prev_far.append(whole(local) >= LANES)
            prev = (
                frame(whole(angles_prev[pl.ds(0, 1), :]), whole(angles_prev[pl.ds(1, 1), :])),
                whole(volume_prev[...]),
                [whole(grad_prev[pl.ds(a, 1), :]) for a in range(4)],
                [whole(grad_prev[pl.ds(4 + a, 1), :]) for a in range(4)],
                prev_low, prev_far,
            )
            own_stress = [stress[pl.ds(k * rows, rows), :] for k in range(3)]
            prev_stress = [whole(stress_prev[pl.ds(k, 1), :]) for k in range(3)]

        def element_forces(batch, tension, near, far):
            (one, two), volume, gx, gy, low, beyond = batch
            corner_vel = [
                [
                    jnp.where(beyond[a], lane_take(far[k], low[a]), lane_take(near[k], low[a]))
                    for a in range(4)
                ]
                for k in range(3)
            ]
            xx = yy = xy = jnp.zeros(volume.shape, F32)
            for a in range(4):
                u = sum(one[k] * corner_vel[k][a] for k in range(3))
                w = sum(two[k] * corner_vel[k][a] for k in range(2))
                xx += gx[a] * u
                yy += gy[a] * w
                xy += gy[a] * u + gx[a] * w
            factor = TIME_STEP * YOUNG_MOD / (1.0 - POISSON * POISSON)
            sxx = tension[0] + factor * (xx + POISSON * yy)
            syy = tension[1] + factor * (POISSON * xx + yy)
            sxy = tension[2] + factor * 0.5 * (1.0 - POISSON) * xy
            hour = [
                HOURGLASS * volume
                * (corner_vel[k][0] - corner_vel[k][1] + corner_vel[k][2] - corner_vel[k][3])
                for k in range(3)
            ]
            forces = []
            for a in range(4):
                f1 = -volume * (gx[a] * sxx + gy[a] * sxy)
                f2 = -volume * (gy[a] * syy + gx[a] * sxy)
                parts = []
                for k in range(3):
                    force = one[k] * f1 - (1.0 if a % 2 == 0 else -1.0) * hour[k]
                    if k < 2:
                        force += two[k] * f2
                    first = force.astype(BF16).astype(F32)
                    parts.append((first, force - first))
                forces.append(parts)
            return [sxx, syy, sxy], forces

        for copy in edge_copies(step):
            copy.wait_recv()
        for k in range(3):
            vel[pl.ds(k * 2 * rows + rows, 1), :] = ghost_recv[step, pl.ds(k, 1), :]
        own_stress, forces = element_forces(
            own, own_stress,
            [velocity_rows(k) for k in range(3)],
            [vel[pl.ds(k * 2 * rows + 1, rows), :] for k in range(3)],
        )
        prev_stress, prev_forces = element_forces(
            prev, prev_stress,
            [whole(last_recv[step, pl.ds(k, 1), :]) for k in range(3)],
            [whole(vel[pl.ds(k * 2 * rows, 1), :]) for k in range(3)],
        )
        for a in range(4):
            for k in range(3):
                for part in range(2):
                    for side in range(2):
                        at = part * 8 + k * 2 + side
                        keep = corner_far[a] if side else jnp.logical_not(corner_far[a])
                        win_rows[a, pl.ds(at, rows, stride=16), :] = jnp.where(
                            keep, forces[a][k][part], 0.0
                        )
                        far_row = jnp.where(prev_far[a], prev_forces[a][k][part], 0.0)[:1]
                        win_rows[a, pl.ds(rows * 16 + at, 1), :] = far_row
        for i in range(rows + 1):
            left = jnp.concatenate(
                [win_rows[a, pl.ds(i * 16, 16), :].astype(BF16) for a in range(4)], axis=1
            )
            summed = nt_dot(left, win_hot[i])
            force_rows[pl.ds(i * 8, 8), :] = summed[:8] + summed[8:]
        internal = []
        for k in range(3):
            near = force_rows[pl.ds(k * 2, rows, stride=8), :]
            far = force_rows[pl.ds(k * 2 + 1, rows - 1, stride=8), :]
            edge_row = force_rows[pl.ds(rows * 8 + k * 2 + 1, 1), :]
            internal.append(near + jnp.concatenate([edge_row, far], axis=0))
        if step + 1 == STEPS:
            for k in range(3):
                for i in range(rows):
                    stress_out[pl.ds(k, 1), pl.ds(i * LANES, LANES)] = own_stress[k][i : i + 1]
        row_iota = lax.broadcasted_iota(jnp.int32, (rows, LANES), 0)
        for n, g in enumerate(arrival):
            if n:
                group_arrival(step, count - n, True).wait_recv()
            source = answer_buf if n else back_buf
            for half in range(halves):
                high = slot_ids[g, pl.ds(half, 1), :] >> 7
                match = row_iota == high
                chosen = jnp.concatenate([
                    jnp.where(
                        match,
                        jnp.broadcast_to(source[step, g, pl.ds(k * halves + half, 1), :], match.shape),
                        0.0,
                    )
                    for k in range(3)
                ], axis=0)
                first = chosen.astype(BF16).astype(F32)
                both = jnp.concatenate([first, chosen - first], axis=0).astype(BF16)
                node_lhs[:, pl.ds((n * halves + half) * LANES, LANES)] = both
        contact = nt_dot(node_lhs[...], node_hot[...])
        contact = contact[: 3 * rows] + contact[3 * rows :]
        for k in range(3):
            fresh = velocity_rows(k) + TIME_STEP * (
                internal[k] + contact[k * rows : (k + 1) * rows]
            ) / mass
            vel[pl.ds(k * 2 * rows, rows), :] = fresh
            pos[pl.ds(k * rows, rows), :] = pos[pl.ds(k * rows, rows), :] + TIME_STEP * fresh
        if step + 1 < STEPS:
            fill_slots(step + 1)
            fill_edges(step + 1)

    for i in range(rows):
        cols = pl.ds(i * LANES, LANES)
        coords_out[:, cols] = pos[pl.ds(i, 3, stride=rows), :]
        velocity_out[:, cols] = vel[pl.ds(i, 3, stride=2 * rows), :]
    for copy in prev_copies():
        copy.wait_send()
    for step in range(STEPS):
        for copy in edge_copies(step):
            copy.wait_send()
        for j in range(count):
            group_copy(step, j, False).wait_send()
            group_copy(step, j, True).wait_send()


def put_out(coords_in, velocity_in, stress_in, coords_out, velocity_out, stress_out, sems):
    pairs = ((coords_in, coords_out), (velocity_in, velocity_out), (stress_in, stress_out))
    copies = [pltpu.make_async_copy(src, dst, sems.at[n]) for n, (src, dst) in enumerate(pairs)]
    for copy in copies:
        copy.start()
    for copy in copies:
        copy.wait()


def per_device(
    sizes, coords, velocity, node_mass, corner_nodes, shape_grad, frame_angles, volume, stress,
    send_nodes, tile_count, tile_nodes, tile_facets, pair_mask,
):
    count = coords.shape[1]
    rows = count // LANES
    group = sizes[1] * sizes[2]
    cap = send_nodes.shape[2]
    tiles = tile_nodes.shape[0]
    spans = group * cap // LANES
    vmem = pl.BlockSpec(memory_space=pltpu.VMEM)
    hbm = pl.BlockSpec(memory_space=pltpu.HBM)
    state = jax.ShapeDtypeStruct((3, count), F32)
    halves = cap // LANES
    arrays = (
        coords, velocity, node_mass.reshape(rows, LANES), corner_nodes, shape_grad, frame_angles,
        volume.reshape(rows, LANES), stress, send_nodes, tile_nodes, tile_facets, pair_mask,
    )
    arrays = tuple(pltpu.with_memory_space_constraint(a, pltpu.HBM) for a in arrays)
    dma = pltpu.SemaphoreType.DMA
    finals = pl.pallas_call(
        functools.partial(kernel, sizes),
        out_shape=(state, state, state),
        in_specs=[hbm] * 12 + [pl.BlockSpec(memory_space=pltpu.SMEM)],
        out_specs=(vmem, vmem, vmem),
        scratch_shapes=[pltpu.VMEM(a.shape, a.dtype) for a in arrays] + [
            dma((len(arrays),)),
            pltpu.VMEM((3 * rows, LANES), F32),
            pltpu.VMEM((6 * rows, LANES), F32),
            pltpu.VMEM((4 * rows, LANES), jnp.int32),
            pltpu.VMEM((8 * rows, LANES), F32),
            pltpu.VMEM((3 * rows, LANES), F32),
            pltpu.VMEM((2 * rows, LANES), F32),
            pltpu.VMEM((group, halves, LANES), jnp.int32),
            pltpu.VMEM((-(-5 * tiles // 8) * 8, LANES), jnp.int32),
            pltpu.VMEM((rows + 1, LANES, 4 * LANES), BF16),
            pltpu.VMEM((LANES, 5 * tiles * LANES), BF16),
            pltpu.VMEM((LANES, group * cap), BF16),
            pltpu.VMEM((4, 16 * (rows + 1), LANES), F32),
            pltpu.VMEM((8 * (rows + 1), LANES), F32),
            pltpu.VMEM((6 * spans, 5 * tiles * LANES), BF16),
            pltpu.VMEM((6 * rows, group * cap), BF16),
            pltpu.VMEM((group, 6 * halves, LANES), F32),
            pltpu.VMEM((group, 6 * halves, LANES), F32),
            pltpu.VMEM((STEPS - 1, group, 3 * halves, LANES), F32),
            pltpu.VMEM((STEPS - 1, group, 3 * halves, LANES), F32),
            pltpu.VMEM((STEPS, group, 3 * halves, LANES), F32),
            pltpu.VMEM((STEPS, group, 3 * halves, LANES), F32),
            pltpu.VMEM((STEPS - 1, 3, LANES), F32),
            pltpu.VMEM((STEPS - 1, 3, LANES), F32),
            pltpu.VMEM((STEPS, 3, LANES), F32),
            pltpu.VMEM((STEPS, 3, LANES), F32),
            pltpu.VMEM((4, LANES), jnp.int32),
            pltpu.VMEM((8, LANES), F32),
            pltpu.VMEM((2, LANES), F32),
            pltpu.VMEM((1, LANES), F32),
            pltpu.VMEM((3, LANES), F32),
            dma((STEPS, group - 1)),
            dma((STEPS, group)),
            dma((STEPS, group - 1)),
            dma((STEPS, group)),
            dma((STEPS, 2)),
            dma((STEPS, 2)),
            dma((5,)),
            dma((5,)),
        ],
        compiler_params=pltpu.CompilerParams(
            collective_id=0, has_side_effects=True, vmem_limit_bytes=24 * 1024 * 1024
        ),
    )(*arrays, tile_count)
    return pl.pallas_call(
        put_out,
        out_shape=(state, state, state),
        in_specs=[vmem] * 3,
        out_specs=(hbm, hbm, hbm),
        scratch_shapes=[dma((3,))],
        compiler_params=pltpu.CompilerParams(vmem_limit_bytes=1024 * 1024),
    )(*finals)


def solution(mesh):
    axes = ("len", "wid", "dep")
    flat, wide = P(axes), P(None, axes)
    sizes = tuple(mesh.shape[name] for name in axes)
    return jax.shard_map(
        functools.partial(per_device, sizes),
        mesh=mesh,
        in_specs=(
            wide, wide, flat, wide, wide, wide, flat, wide,
            P(axes, None, None), flat, P(axes, None), P(None, axes, None), P(axes, None, None),
        ),
        out_specs=(wide, wide, wide),
        check_vma=False,
    )
```

```python
import functools

import jax
import jax.numpy as jnp
from jax import lax
from jax.experimental import pallas as pl
from jax.experimental.pallas import tpu as pltpu
from jax.sharding import PartitionSpec as P

STEPS = 2
TIME_STEP = 0.1
YOUNG_MOD = 1.0
POISSON = 0.3
HOURGLASS = 0.1
RADIUS_SQ = 1.0
STIFFNESS = 0.1
DAMPING = 0.05

LANES = 128
MESH = pl.DeviceIdType.MESH
F32 = jnp.float32
BF16 = jnp.bfloat16


def two_parts(values):
    first = values.astype(BF16)
    return first, (values - first.astype(F32)).astype(BF16)


def lane_take(table, low):
    return jnp.take_along_axis(table, low, axis=1, mode="promise_in_bounds")


def nt_dot(left, right):
    return lax.dot_general(left, right, (((1,), (1,)), ((), ())), preferred_element_type=F32)


def nn_dot(left, right):
    return lax.dot_general(left, right, (((1,), (0,)), ((), ())), preferred_element_type=F32)


def kernel(
    sizes,
    coords_hbm, velocity_hbm, mass_hbm, corner_hbm, grad_hbm, angles_hbm, volume_hbm, stress_hbm,
    send_hbm, nodes_hbm, facets_hbm, mask_hbm, count_in,
    coords_out, velocity_out, stress_out,
    coords_in, velocity_in, mass_in, corner_in, grad_in, angles_in, volume_in, stress_in,
    send_in, nodes_in, facets_in, mask_in, in_sem,
    pos, vel, corner, grad, stress, angle, slot_ids, tile_ids, win_hot, look_hot, slot_hot, node_hot,
    win_rows, force_rows, tile_lhs, pairs, column_buf,
    send_buf, recv_buf, again_buf, fresh_buf, back_buf, answer_buf,
    first_buf, last_buf, ghost_recv, last_recv,
    corner_prev, grad_prev, angles_prev, volume_prev, stress_prev,
    out_send_sem, out_recv_sem, back_send_sem, back_recv_sem, edge_send_sem, edge_recv_sem,
    prev_send_sem, prev_recv_sem,
):
    n_len, n_wid, n_dep = sizes
    group = n_wid * n_dep
    devices = n_len * group
    rows = coords_in.shape[1] // LANES
    cap = send_in.shape[2]
    halves = cap // LANES
    tiles = nodes_in.shape[0]
    my_len = lax.axis_index("len")
    my_wid = lax.axis_index("wid")
    my_dep = lax.axis_index("dep")
    my_place = my_wid * n_dep + my_dep
    my_id = my_len * group + my_place

    def by_id(p):
        return (p // group, (p % group) // n_dep, p % n_dep)

    upper = (2 * my_wid) // n_wid
    shifts = sorted(range(1, n_dep), key=lambda d: -min(d, n_dep - d))
    peers = []
    for r in range(n_wid):
        across = r + (1 - upper) * (n_wid - 1 - 2 * r)
        for shift in shifts:
            peers.append((across, lax.rem(my_dep + shift, n_dep)))
        if r < n_wid - 1:
            up = r + (r - my_wid + n_wid) // n_wid
            down = n_wid - 1 - r - (my_wid - (n_wid - 1 - r) + n_wid) // n_wid
            peers.append((upper * up + (1 - upper) * down, my_dep))
    places = [wid * n_dep + dep for wid, dep in peers]
    count = group - 1
    arrival = [my_place] + places[::-1]

    before = by_id(lax.rem(my_id + devices - 1, devices))
    after = by_id(lax.rem(my_id + 1, devices))

    loads = [
        pltpu.make_async_copy(src, dst, in_sem.at[n])
        for n, (src, dst) in enumerate((
            (send_hbm, send_in), (velocity_hbm, velocity_in), (coords_hbm, coords_in),
            (corner_hbm, corner_in), (stress_hbm, stress_in), (grad_hbm, grad_in),
            (angles_hbm, angles_in), (mass_hbm, mass_in), (volume_hbm, volume_in),
            (nodes_hbm, nodes_in), (facets_hbm, facets_in), (mask_hbm, mask_in),
        ))
    ]
    for load in loads[:3]:
        load.start()
    barrier = pltpu.get_barrier_semaphore()
    for wid, dep in peers:
        pl.semaphore_signal(barrier, inc=1, device_id=(my_len, wid, dep), device_id_type=MESH)
    pl.semaphore_signal(barrier, inc=1, device_id=before, device_id_type=MESH)
    pl.semaphore_signal(barrier, inc=1, device_id=after, device_id_type=MESH)
    for load in loads[3:]:
        load.start()
    for load in loads[:3]:
        load.wait()
    for i in range(rows):
        cols = pl.ds(i * LANES, LANES)
        pos[pl.ds(i, 3, stride=rows), :] = coords_in[:, cols]
        for k in range(3):
            vel[pl.ds(k * 2 * rows + i, 1), :] = velocity_in[pl.ds(k, 1), cols]

    def velocity_rows(k):
        return vel[pl.ds(k * 2 * rows, rows), :]

    def fill_edges(step):
        for k in range(3):
            first_buf[step - 1, pl.ds(k, 1), :] = vel[pl.ds(k * 2 * rows, 1), :]
            last_buf[step - 1, pl.ds(k, 1), :] = vel[pl.ds(k * 2 * rows + rows - 1, 1), :]

    segment = group // 2
    bases = [pl.multiple_of(side * segment, segment) for side in (1 - upper, upper)]

    def fill_slots(step, base):
        tables = [velocity_rows(k) for k in range(3)]
        if step == 0:
            tables += [pos[pl.ds(k * rows, rows), :] for k in range(3)]
        target = send_buf if step == 0 else again_buf.at[step - 1]
        for half in range(halves):
            cols = pl.ds(half * LANES, LANES)
            ids = send_in[0, pl.ds(base, segment), cols]
            low, high = ids & (LANES - 1), ids >> 7
            if step == 0:
                slot_ids[pl.ds(base, segment), half, :] = high
            for c, table in enumerate(tables):
                found = jnp.zeros(ids.shape, F32)
                for h in range(rows):
                    row = jnp.broadcast_to(table[h : h + 1], ids.shape)
                    found = jnp.where(high == h, lane_take(row, low), found)
                target[pl.ds(base, segment), c, cols] = found

    def remote(src, dst, send_sem, recv_sem, target):
        return pltpu.make_async_remote_copy(
            src_ref=src, dst_ref=dst, send_sem=send_sem, recv_sem=recv_sem,
            device_id=target, device_id_type=MESH,
        )

    final = pl.ds((rows - 1) * LANES, LANES)

    def edge_copies(step):
        if step == 0:
            first, last = velocity_in.at[:, pl.ds(0, LANES)], velocity_in.at[:, final]
        else:
            first, last = first_buf.at[step - 1], last_buf.at[step - 1]
        return (
            remote(first, ghost_recv.at[step], edge_send_sem.at[step, 0], edge_recv_sem.at[step, 0], before),
            remote(last, last_recv.at[step], edge_send_sem.at[step, 1], edge_recv_sem.at[step, 1], after),
        )

    def prev_copies():
        pairs = (
            (corner_in.at[:, final], corner_prev), (grad_in.at[:, final], grad_prev),
            (angles_in.at[:, final], angles_prev), (stress_in.at[:, final], stress_prev),
            (volume_in.at[pl.ds(rows - 1, 1), :], volume_prev),
        )
        return [
            remote(src, dst, prev_send_sem.at[n], prev_recv_sem.at[n], after)
            for n, (src, dst) in enumerate(pairs)
        ]

    def ends(step, back):
        if back:
            return back_buf.at[step], answer_buf.at[step], back_send_sem, back_recv_sem, 3
        if step == 0:
            return send_buf, recv_buf, out_send_sem, out_recv_sem, 6
        return again_buf.at[step - 1], fresh_buf.at[step - 1], out_send_sem, out_recv_sem, 3

    def group_copy(step, j, back, arriving=False):
        wid, dep = peers[j]
        src, dst, ss, rs, depth = ends(step, back)
        slot = places[j] if arriving else my_place
        return remote(
            src.at[places[j], pl.ds(0, depth)], dst.at[slot, pl.ds(0, depth)],
            ss.at[step, j], rs.at[step, slot], (my_len, wid, dep),
        )

    batch = group // 2
    far_count = n_dep * (n_wid // 2)
    parts = ((bases[0], range(far_count)), (bases[1], range(far_count, count)))

    fill_slots(0, bases[0])
    pl.semaphore_wait(barrier, group + 1)

    sub = lax.broadcasted_iota(jnp.int32, (LANES, LANES), 0)
    lane = lax.broadcasted_iota(jnp.int32, (LANES, LANES), 1)
    lane_tall = lax.broadcasted_iota(jnp.int32, (cap, LANES), 1)
    eight = lax.broadcasted_iota(jnp.int32, (8, LANES), 0)
    row_iota = lax.broadcasted_iota(jnp.int32, (rows, LANES), 0)
    group_iota = lax.broadcasted_iota(jnp.int32, (group, LANES), 0)

    def split(values):
        first = values.astype(BF16).astype(F32)
        return first, values - first

    for step in range(STEPS):
        for base, span in parts:
            if step or base is not bases[0]:
                fill_slots(step, base)
            for j in span:
                group_copy(step, j, False).start()
        if step:
            fill_edges(step)
        for copy in edge_copies(step):
            copy.start()

        if step == 0:
            for load in loads[3:]:
                load.wait()
            for copy in prev_copies():
                copy.start()
            for i in range(rows):
                cols = pl.ds(i * LANES, LANES)
                stress[pl.ds(i, 3, stride=rows), :] = stress_in[:, cols]
                corner[pl.ds(i, 4, stride=rows), :] = corner_in[:, cols]
                grad[pl.ds(i, 8, stride=rows), :] = grad_in[:, cols]
                angle[pl.ds(i, 2, stride=rows), :] = angles_in[:, cols]
            tile_ids[...] = jnp.zeros_like(tile_ids)
            tile_ids[pl.ds(0, tiles), :] = nodes_in[...]
            for a in range(4):
                tile_ids[pl.ds((a + 1) * tiles, tiles), :] = facets_in[a]
            first_row = lax.broadcasted_iota(jnp.int32, (rows, LANES), 0) * LANES
            corner_low, corner_far = [], []
            for a in range(4):
                local = corner[pl.ds(a * rows, rows), :] - first_row
                corner_low.append(local & (LANES - 1))
                corner_far.append(local >= LANES)
                for i in range(rows):
                    hot = (sub == corner_low[a][i : i + 1]).astype(F32).astype(BF16)
                    win_hot[i, :, pl.ds(a * LANES, LANES)] = hot
            polar, azim = angle[pl.ds(0, rows), :], angle[pl.ds(rows, rows), :]

            def frame(polar, azim):
                cos_p, sin_p, cos_a, sin_a = jnp.cos(polar), jnp.sin(polar), jnp.cos(azim), jnp.sin(azim)
                return (cos_p * cos_a, cos_p * sin_a, -sin_p), (-sin_a, cos_a)

            volume = volume_in[...]
            mass = mass_in[...]
            gx = [grad[pl.ds(a * rows, rows), :] for a in range(4)]
            gy = [grad[pl.ds((4 + a) * rows, rows), :] for a in range(4)]
            own = (frame(polar, azim), volume, gx, gy, corner_low, corner_far)
            slots_high = tile_ids[...] // cap
            slots_low = tile_ids[...] % cap
            low_columns = jnp.transpose(slots_low)
            node_columns = jnp.transpose(send_in[0] & (LANES - 1))
            for g in range(group):
                column_buf[pl.ds(g * cap, cap), :] = jnp.broadcast_to(node_columns[:, g : g + 1], (cap, LANES))
            for b in range(5 * tiles):
                cols = pl.ds(b * LANES, LANES)
                for half in range(halves):
                    span = pl.ds(half * LANES, LANES)
                    hot = sub + half * LANES == slots_low[b : b + 1]
                    look_hot[span, cols] = hot.astype(F32).astype(BF16)
                    hot = lane + half * LANES == low_columns[:, b : b + 1]
                    slot_hot[cols, span] = hot.astype(F32).astype(BF16)
            for n, g in enumerate(arrival):
                hot = lane_tall == column_buf[pl.ds(pl.multiple_of(g * cap, cap), cap), :]
                node_hot[pl.ds(n * cap, cap), :] = hot.astype(F32).astype(BF16)

        mine, landed = (send_buf, recv_buf) if step == 0 else (again_buf.at[step - 1], fresh_buf.at[step - 1])
        landed[my_place] = mine[my_place]
        for j in range(count)[::-1]:
            group_copy(step, j, False, True).wait_recv()
        table = []
        for g in range(group):
            table += [part.astype(BF16) for part in split(landed[g])]
        table = jnp.concatenate(table, axis=0)
        state = []
        for b in range(0, 5 * tiles, 2):
            looked = nn_dot(table, look_hot[:, pl.ds(b * LANES, 2 * LANES)])
            for side in range(2):
                high = jnp.broadcast_to(slots_high[b + side : b + side + 1], (8, LANES))
                block = looked[:, side * LANES : (side + 1) * LANES]
                first, second = block[:8], block[8:16]
                for g in range(1, group):
                    match = high == g
                    first = jnp.where(match, block[g * 16 : g * 16 + 8], first)
                    second = jnp.where(match, block[g * 16 + 8 : g * 16 + 16], second)
                state.append(first + second)
        bodies = state[:tiles] + [
            0.25 * sum(state[(a + 1) * tiles + t] for a in range(4)) for t in range(tiles)
        ]
        if step:
            bodies = [
                jnp.where(eight < 3, new, old + TIME_STEP * jnp.roll(new, 3, axis=0))
                for new, old in zip(bodies, old_bodies)
            ]
        old_bodies = bodies
        mixes = [
            jnp.where(eight < 3, STIFFNESS * jnp.roll(body, 5, axis=0) - DAMPING * body, 0.0)
            for body in bodies
        ]
        sides = [jnp.where(eight == 3, 1.0, mix) for mix in mixes]
        columns = jnp.transpose(jnp.concatenate(bodies[:tiles], axis=0))
        forces = []
        for t in range(tiles):
            live = jnp.where(t < count_in[0], 1.0, 0.0)
            dist = jnp.zeros((LANES, LANES), F32)
            for k in range(3, 6):
                gap = columns[:, 8 * t + k : 8 * t + k + 1] - bodies[tiles + t][k : k + 1]
                dist += gap * gap
            weight = mask_in[t].astype(F32) * (live * jnp.maximum(RADIUS_SQ - dist, 0.0))
            w1, w2 = two_parts(weight)
            left_a = jnp.concatenate(two_parts(sides[t]), axis=0)
            left_b = jnp.concatenate(two_parts(sides[tiles + t]), axis=0)
            to_facet = nn_dot(
                jnp.concatenate([left_a, left_a], axis=1), jnp.concatenate([w1, w2], axis=0)
            )
            to_node = nt_dot(
                jnp.concatenate([left_b, left_b], axis=1), jnp.concatenate([w1, w2], axis=1)
            )
            to_facet = to_facet[:8] + to_facet[8:]
            to_node = to_node[:8] + to_node[8:]
            node_force = mixes[t] * to_node[3:4] - to_node
            facet_force = -0.25 * (to_facet - to_facet[3:4] * mixes[tiles + t])
            for force, blocks in ((node_force, [t]), (facet_force, [(a + 1) * tiles + t for a in range(4)])):
                matches = [group_iota == slots_high[b : b + 1] for b in blocks]
                for part, value in enumerate(split(force)):
                    for k in range(3):
                        row = jnp.broadcast_to(value[k : k + 1], (group, LANES))
                        for b, match in zip(blocks, matches):
                            tile_lhs[pl.ds((part * 3 + k) * group, group), pl.ds(b * LANES, LANES)] = (
                                jnp.where(match, row, 0.0).astype(BF16)
                            )
        slots = nn_dot(tile_lhs[...], slot_hot[...])
        slots = slots[: 3 * group] + slots[3 * group :]
        for k in range(3):
            back_buf[step, :, k, :] = slots[k * group : (k + 1) * group]
        for j in range(count):
            group_copy(step, j, True).start()

        if step == 0:
            for copy in prev_copies():
                copy.wait_recv()

            def whole(row):
                return jnp.broadcast_to(row, (8, LANES))

            prev_low, prev_far = [], []
            for a in range(4):
                local = corner_prev[pl.ds(a, 1), :] - (rows - 1) * LANES
                low = local & (LANES - 1)
                win_hot[rows, :, pl.ds(a * LANES, LANES)] = (sub == low).astype(F32).astype(BF16)
                prev_low.append(whole(low))
                prev_far.append(whole(local) >= LANES)
            prev = (
                frame(whole(angles_prev[pl.ds(0, 1), :]), whole(angles_prev[pl.ds(1, 1), :])),
                whole(volume_prev[...]),
                [whole(grad_prev[pl.ds(a, 1), :]) for a in range(4)],
                [whole(grad_prev[pl.ds(4 + a, 1), :]) for a in range(4)],
                prev_low, prev_far,
            )
            own_stress = [stress[pl.ds(k * rows, rows), :] for k in range(3)]
            prev_stress = [whole(stress_prev[pl.ds(k, 1), :]) for k in range(3)]

        def element_forces(batch, tension, near, far):
            (one, two), volume, gx, gy, low, beyond = batch
            corner_vel = [
                [
                    jnp.where(beyond[a], lane_take(far[k], low[a]), lane_take(near[k], low[a]))
                    for a in range(4)
                ]
                for k in range(3)
            ]
            xx = yy = xy = jnp.zeros(volume.shape, F32)
            for a in range(4):
                u = sum(one[k] * corner_vel[k][a] for k in range(3))
                w = sum(two[k] * corner_vel[k][a] for k in range(2))
                xx += gx[a] * u
                yy += gy[a] * w
                xy += gy[a] * u + gx[a] * w
            factor = TIME_STEP * YOUNG_MOD / (1.0 - POISSON * POISSON)
            sxx = tension[0] + factor * (xx + POISSON * yy)
            syy = tension[1] + factor * (POISSON * xx + yy)
            sxy = tension[2] + factor * 0.5 * (1.0 - POISSON) * xy
            hour = [
                HOURGLASS * volume
                * (corner_vel[k][0] - corner_vel[k][1] + corner_vel[k][2] - corner_vel[k][3])
                for k in range(3)
            ]
            forces = []
            for a in range(4):
                f1 = -volume * (gx[a] * sxx + gy[a] * sxy)
                f2 = -volume * (gy[a] * syy + gx[a] * sxy)
                parts = []
                for k in range(3):
                    force = one[k] * f1 - (1.0 if a % 2 == 0 else -1.0) * hour[k]
                    if k < 2:
                        force += two[k] * f2
                    first = force.astype(BF16).astype(F32)
                    parts.append((first, force - first))
                forces.append(parts)
            return [sxx, syy, sxy], forces

        for copy in edge_copies(step):
            copy.wait_recv()
        for k in range(3):
            vel[pl.ds(k * 2 * rows + rows, 1), :] = ghost_recv[step, pl.ds(k, 1), :]
        own_stress, forces = element_forces(
            own, own_stress,
            [velocity_rows(k) for k in range(3)],
            [vel[pl.ds(k * 2 * rows + 1, rows), :] for k in range(3)],
        )
        prev_stress, prev_forces = element_forces(
            prev, prev_stress,
            [whole(last_recv[step, pl.ds(k, 1), :]) for k in range(3)],
            [whole(vel[pl.ds(k * 2 * rows, 1), :]) for k in range(3)],
        )
        for a in range(4):
            for k in range(3):
                for part in range(2):
                    for side in range(2):
                        at = part * 8 + k * 2 + side
                        keep = corner_far[a] if side else jnp.logical_not(corner_far[a])
                        win_rows[a, pl.ds(at, rows, stride=16), :] = jnp.where(
                            keep, forces[a][k][part], 0.0
                        )
                        far_row = jnp.where(prev_far[a], prev_forces[a][k][part], 0.0)[:1]
                        win_rows[a, pl.ds(rows * 16 + at, 1), :] = far_row
        for i in range(rows + 1):
            left = jnp.concatenate(
                [win_rows[a, pl.ds(i * 16, 16), :].astype(BF16) for a in range(4)], axis=1
            )
            summed = nt_dot(left, win_hot[i])
            force_rows[pl.ds(i * 8, 8), :] = summed[:8] + summed[8:]
        internal = []
        for k in range(3):
            near = force_rows[pl.ds(k * 2, rows, stride=8), :]
            far = force_rows[pl.ds(k * 2 + 1, rows - 1, stride=8), :]
            edge_row = force_rows[pl.ds(rows * 8 + k * 2 + 1, 1), :]
            internal.append(near + jnp.concatenate([edge_row, far], axis=0))
        if step + 1 == STEPS:
            for k in range(3):
                for i in range(rows):
                    stress_out[pl.ds(k, 1), pl.ds(i * LANES, LANES)] = own_stress[k][i : i + 1]
        contact = jnp.zeros((3 * rows, LANES), F32)
        for begin in range(0, group, batch):
            for n in range(max(begin, 1), begin + batch):
                group_copy(step, count - n, True, True).wait_recv()
            for n in range(begin, begin + batch):
                g = arrival[n]
                source = answer_buf if n else back_buf
                halved = split(source[step, g])
                for half in range(halves):
                    match = row_iota == slot_ids[g, pl.ds(half, 1), :]
                    at = pl.ds((n * halves + half) * LANES, LANES)
                    for part in range(2):
                        for k in range(3):
                            row = halved[part][k : k + 1, half * LANES : (half + 1) * LANES]
                            chosen = jnp.where(match, jnp.broadcast_to(row, match.shape), 0.0)
                            pairs[pl.ds((part * 3 + k) * rows, rows), at] = chosen.astype(BF16)
            at = pl.ds(begin * cap, batch * cap)
            summed = nn_dot(pairs[:, at], node_hot[at, :])
            contact += summed[: 3 * rows] + summed[3 * rows :]
        for k in range(3):
            fresh = velocity_rows(k) + TIME_STEP * (
                internal[k] + contact[k * rows : (k + 1) * rows]
            ) / mass
            vel[pl.ds(k * 2 * rows, rows), :] = fresh
            pos[pl.ds(k * rows, rows), :] = pos[pl.ds(k * rows, rows), :] + TIME_STEP * fresh

    for i in range(rows):
        cols = pl.ds(i * LANES, LANES)
        coords_out[:, cols] = pos[pl.ds(i, 3, stride=rows), :]
        velocity_out[:, cols] = vel[pl.ds(i, 3, stride=2 * rows), :]
    for copy in prev_copies():
        copy.wait_send()
    for step in range(STEPS):
        for copy in edge_copies(step):
            copy.wait_send()
        for j in range(count):
            group_copy(step, j, False).wait_send()
            group_copy(step, j, True).wait_send()


def put_out(coords_in, velocity_in, stress_in, coords_out, velocity_out, stress_out, sems):
    pairs = ((coords_in, coords_out), (velocity_in, velocity_out), (stress_in, stress_out))
    copies = [pltpu.make_async_copy(src, dst, sems.at[n]) for n, (src, dst) in enumerate(pairs)]
    for copy in copies:
        copy.start()
    for copy in copies:
        copy.wait()


def per_device(
    sizes, coords, velocity, node_mass, corner_nodes, shape_grad, frame_angles, volume, stress,
    send_nodes, tile_count, tile_nodes, tile_facets, pair_mask,
):
    count = coords.shape[1]
    rows = count // LANES
    group = sizes[1] * sizes[2]
    cap = send_nodes.shape[2]
    tiles = tile_nodes.shape[0]
    vmem = pl.BlockSpec(memory_space=pltpu.VMEM)
    hbm = pl.BlockSpec(memory_space=pltpu.HBM)
    state = jax.ShapeDtypeStruct((3, count), F32)
    halves = cap // LANES
    arrays = (
        coords, velocity, node_mass.reshape(rows, LANES), corner_nodes, shape_grad, frame_angles,
        volume.reshape(rows, LANES), stress, send_nodes, tile_nodes, tile_facets, pair_mask,
    )
    arrays = tuple(pltpu.with_memory_space_constraint(a, pltpu.HBM) for a in arrays)
    dma = pltpu.SemaphoreType.DMA
    finals = pl.pallas_call(
        functools.partial(kernel, sizes),
        out_shape=(state, state, state),
        in_specs=[hbm] * 12 + [pl.BlockSpec(memory_space=pltpu.SMEM)],
        out_specs=(vmem, vmem, vmem),
        scratch_shapes=[pltpu.VMEM(a.shape, a.dtype) for a in arrays] + [
            dma((len(arrays),)),
            pltpu.VMEM((3 * rows, LANES), F32),
            pltpu.VMEM((6 * rows, LANES), F32),
            pltpu.VMEM((4 * rows, LANES), jnp.int32),
            pltpu.VMEM((8 * rows, LANES), F32),
            pltpu.VMEM((3 * rows, LANES), F32),
            pltpu.VMEM((2 * rows, LANES), F32),
            pltpu.VMEM((group, halves, LANES), jnp.int32),
            pltpu.VMEM((-(-5 * tiles // 8) * 8, LANES), jnp.int32),
            pltpu.VMEM((rows + 1, LANES, 4 * LANES), BF16),
            pltpu.VMEM((cap, 5 * tiles * LANES), BF16),
            pltpu.VMEM((5 * tiles * LANES, cap), BF16),
            pltpu.VMEM((group * cap, LANES), BF16),
            pltpu.VMEM((4, 16 * (rows + 1), LANES), F32),
            pltpu.VMEM((8 * (rows + 1), LANES), F32),
            pltpu.VMEM((6 * group, 5 * tiles * LANES), BF16),
            pltpu.VMEM((6 * rows, group * cap), BF16),
            pltpu.VMEM((group * cap, LANES), jnp.int32),
            pltpu.VMEM((group, 8, cap), F32),
            pltpu.VMEM((group, 8, cap), F32),
            pltpu.VMEM((STEPS - 1, group, 8, cap), F32),
            pltpu.VMEM((STEPS - 1, group, 8, cap), F32),
            pltpu.VMEM((STEPS, group, 4, cap), F32),
            pltpu.VMEM((STEPS, group, 4, cap), F32),
            pltpu.VMEM((STEPS - 1, 3, LANES), F32),
            pltpu.VMEM((STEPS - 1, 3, LANES), F32),
            pltpu.VMEM((STEPS, 3, LANES), F32),
            pltpu.VMEM((STEPS, 3, LANES), F32),
            pltpu.VMEM((4, LANES), jnp.int32),
            pltpu.VMEM((8, LANES), F32),
            pltpu.VMEM((2, LANES), F32),
            pltpu.VMEM((1, LANES), F32),
            pltpu.VMEM((3, LANES), F32),
            dma((STEPS, group - 1)),
            dma((STEPS, group)),
            dma((STEPS, group - 1)),
            dma((STEPS, group)),
            dma((STEPS, 2)),
            dma((STEPS, 2)),
            dma((5,)),
            dma((5,)),
        ],
        compiler_params=pltpu.CompilerParams(
            collective_id=0, has_side_effects=True, vmem_limit_bytes=24 * 1024 * 1024
        ),
    )(*arrays, tile_count)
    return pl.pallas_call(
        put_out,
        out_shape=(state, state, state),
        in_specs=[vmem] * 3,
        out_specs=(hbm, hbm, hbm),
        scratch_shapes=[dma((3,))],
        compiler_params=pltpu.CompilerParams(vmem_limit_bytes=1024 * 1024),
    )(*finals)


def solution(mesh):
    axes = ("len", "wid", "dep")
    flat, wide = P(axes), P(None, axes)
    sizes = tuple(mesh.shape[name] for name in axes)
    return jax.shard_map(
        functools.partial(per_device, sizes),
        mesh=mesh,
        in_specs=(
            wide, wide, flat, wide, wide, wide, flat, wide,
            P(axes, None, None), flat, P(axes, None), P(None, axes, None), P(axes, None, None),
        ),
        out_specs=(wide, wide, wide),
        check_vma=False,
    )
```

```python
import functools

import jax
import jax.numpy as jnp
from jax import lax
from jax.experimental import pallas as pl
from jax.experimental.pallas import tpu as pltpu
from jax.sharding import PartitionSpec as P

STEPS = 2
TIME_STEP = 0.1
YOUNG_MOD = 1.0
POISSON = 0.3
HOURGLASS = 0.1
RADIUS_SQ = 1.0
STIFFNESS = 0.1
DAMPING = 0.05

LANES = 128
MESH = pl.DeviceIdType.MESH
F32 = jnp.float32
BF16 = jnp.bfloat16
F8 = jnp.float8_e4m3fn


def two_parts(values):
    first = values.astype(BF16)
    return first, (values - first.astype(F32)).astype(BF16)


def lane_take(table, low):
    return jnp.take_along_axis(table, low, axis=1, mode="promise_in_bounds")


def nt_dot(left, right):
    return lax.dot_general(left, right, (((1,), (1,)), ((), ())), preferred_element_type=F32)


def nn_dot(left, right):
    return lax.dot_general(left, right, (((1,), (0,)), ((), ())), preferred_element_type=F32)


def kernel(
    sizes,
    coords_hbm, velocity_hbm, mass_hbm, corner_hbm, grad_hbm, angles_hbm, volume_hbm, stress_hbm,
    send_hbm, nodes_hbm, facets_hbm, mask_hbm, count_in,
    coords_out, velocity_out, stress_out,
    coords_in, velocity_in, mass_in, corner_in, grad_in, angles_in, volume_in, stress_in,
    send_in, nodes_in, facets_in, mask_in, in_sem,
    pos, vel, corner, grad, stress, angle, slot_ids, tile_ids, win_hot, look_hot, slot_hot, node_hot,
    win_rows, force_rows, tile_lhs, pairs, column_buf, weight_in,
    send_buf, recv_buf, again_buf, fresh_buf, back_buf, answer_buf,
    first_buf, last_buf, edge_recv,
    corner_prev, grad_prev, angles_prev, volume_prev, stress_prev,
    send_sem, out_sem, back_sem, edge_sem, prev_sem,
):
    n_len, n_wid, n_dep = sizes
    group = n_wid * n_dep
    devices = n_len * group
    rows = coords_in.shape[1] // LANES
    cap = send_in.shape[2]
    halves = cap // LANES
    tiles = nodes_in.shape[0]
    my_len = lax.axis_index("len")
    my_wid = lax.axis_index("wid")
    my_dep = lax.axis_index("dep")
    my_place = my_wid * n_dep + my_dep
    my_id = my_len * group + my_place

    def by_id(p):
        return (p // group, (p % group) // n_dep, p % n_dep)

    upper = (2 * my_wid) // n_wid
    shifts = sorted(range(1, n_dep), key=lambda d: -min(d, n_dep - d))
    peers = []
    for r in range(n_wid):
        across = r + (1 - upper) * (n_wid - 1 - 2 * r)
        for shift in shifts:
            peers.append((across, lax.rem(my_dep + shift, n_dep)))
        if r < n_wid - 1:
            up = r + (r - my_wid + n_wid) // n_wid
            down = n_wid - 1 - r - (my_wid - (n_wid - 1 - r) + n_wid) // n_wid
            peers.append((upper * up + (1 - upper) * down, my_dep))
    places = [wid * n_dep + dep for wid, dep in peers]
    count = group - 1
    arrival = [my_place] + places[::-1]

    before = by_id(lax.rem(my_id + devices - 1, devices))
    after = by_id(lax.rem(my_id + 1, devices))

    loads = [
        pltpu.make_async_copy(src, dst, in_sem.at[n])
        for n, (src, dst) in enumerate((
            (send_hbm, send_in), (velocity_hbm, velocity_in), (coords_hbm, coords_in),
            (corner_hbm, corner_in), (stress_hbm, stress_in), (grad_hbm, grad_in),
            (angles_hbm, angles_in), (mass_hbm, mass_in), (volume_hbm, volume_in),
            (nodes_hbm, nodes_in), (facets_hbm, facets_in), (mask_hbm, mask_in),
        ))
    ]
    barrier = pltpu.get_barrier_semaphore()
    for wid, dep in peers:
        pl.semaphore_signal(barrier, inc=1, device_id=(my_len, wid, dep), device_id_type=MESH)
    pl.semaphore_signal(barrier, inc=1, device_id=before, device_id_type=MESH)
    pl.semaphore_signal(barrier, inc=1, device_id=after, device_id_type=MESH)
    for load in loads:
        load.start()
    for load in loads[:3]:
        load.wait()
    for i in range(rows):
        cols = pl.ds(i * LANES, LANES)
        pos[pl.ds(i, 3, stride=rows), :] = coords_in[:, cols]
        for k in range(3):
            vel[pl.ds(k * 2 * rows + i, 1), :] = velocity_in[pl.ds(k, 1), cols]

    def velocity_rows(k):
        return vel[pl.ds(k * 2 * rows, rows), :]

    def fill_edges(step):
        for k in range(3):
            first_buf[step - 1, pl.ds(k, 1), :] = vel[pl.ds(k * 2 * rows, 1), :]
            last_buf[step - 1, pl.ds(k, 1), :] = vel[pl.ds(k * 2 * rows + rows - 1, 1), :]

    segment = group // 2
    bases = [pl.multiple_of(side * segment, segment) for side in (1 - upper, upper)]

    def fill_slots(step, base):
        tables = [velocity_rows(k) for k in range(3)]
        if step == 0:
            tables += [pos[pl.ds(k * rows, rows), :] for k in range(3)]
        target = send_buf if step == 0 else again_buf.at[step - 1]
        for half in range(halves):
            cols = pl.ds(half * LANES, LANES)
            ids = send_in[0, pl.ds(base, segment), cols]
            low, high = ids & (LANES - 1), ids >> 7
            if step == 0:
                slot_ids[pl.ds(base, segment), half, :] = high
            for c, table in enumerate(tables):
                found = jnp.zeros(ids.shape, F32)
                for h in range(rows):
                    row = jnp.broadcast_to(table[h : h + 1], ids.shape)
                    found = jnp.where(high == h, lane_take(row, low), found)
                target[pl.ds(base, segment), c, cols] = found

    def remote(src, dst, recv_sem, target):
        return pltpu.make_async_remote_copy(
            src_ref=src, dst_ref=dst, send_sem=send_sem.at[0], recv_sem=recv_sem,
            device_id=target, device_id_type=MESH,
        )

    def drain(ref, sem):
        pltpu.make_async_copy(ref, ref, sem).wait()

    final = pl.ds((rows - 1) * LANES, LANES)

    def edge_copies(step):
        if step == 0:
            first, last = velocity_in.at[:, pl.ds(0, LANES)], velocity_in.at[:, final]
        else:
            first, last = first_buf.at[step - 1], last_buf.at[step - 1]
        return (
            remote(first, edge_recv.at[step, 0], edge_sem.at[step], before),
            remote(last, edge_recv.at[step, 1], edge_sem.at[step], after),
        )

    def prev_copies():
        pairs = (
            (corner_in.at[:, final], corner_prev), (grad_in.at[:, final], grad_prev),
            (angles_in.at[:, final], angles_prev), (stress_in.at[:, final], stress_prev),
            (volume_in.at[pl.ds(rows - 1, 1), :], volume_prev),
        )
        return [
            remote(src, dst, prev_sem.at[0], after) for src, dst in pairs
        ]

    far_count = n_dep * (n_wid // 2)

    def group_copy(step, j, back):
        wid, dep = peers[j]
        if back:
            src, dst, depth, sem = back_buf.at[step], answer_buf.at[step], 3, back_sem.at[step, int(j < far_count)]
        elif step == 0:
            src, dst, depth, sem = send_buf, recv_buf, 6, out_sem.at[step]
        else:
            src, dst, depth, sem = again_buf.at[step - 1], fresh_buf.at[step - 1], 3, out_sem.at[step]
        return remote(
            src.at[places[j], pl.ds(0, depth)], dst.at[my_place, pl.ds(0, depth)], sem, (my_len, wid, dep)
        )

    batch = count + 1 - far_count
    parts = ((bases[0], range(far_count)), (bases[1], range(far_count, count)))

    fill_slots(0, bases[0])
    pl.semaphore_wait(barrier, group + 1)

    sub = lax.broadcasted_iota(jnp.int32, (LANES, LANES), 0)
    lane = lax.broadcasted_iota(jnp.int32, (LANES, LANES), 1)
    lane_tall = lax.broadcasted_iota(jnp.int32, (cap, LANES), 1)
    eight = lax.broadcasted_iota(jnp.int32, (8, LANES), 0)
    row_iota = lax.broadcasted_iota(jnp.int32, (rows, LANES), 0)
    eight_wide = lax.broadcasted_iota(jnp.int32, (8, cap), 0)
    group_iota = lax.broadcasted_iota(jnp.int32, (group, LANES), 0)

    def split(values):
        first = values.astype(BF16).astype(F32)
        return first, values - first

    for step in range(STEPS):
        for base, span in parts:
            if step or base is not bases[0]:
                fill_slots(step, base)
            for j in span:
                group_copy(step, j, False).start()
        if step:
            fill_edges(step)
        for copy in edge_copies(step):
            copy.start()

        if step == 0:
            for load in loads[3:]:
                load.wait()
            for copy in prev_copies():
                copy.start()
            for i in range(rows):
                cols = pl.ds(i * LANES, LANES)
                stress[pl.ds(i, 3, stride=rows), :] = stress_in[:, cols]
                corner[pl.ds(i, 4, stride=rows), :] = corner_in[:, cols]
                grad[pl.ds(i, 8, stride=rows), :] = grad_in[:, cols]
                angle[pl.ds(i, 2, stride=rows), :] = angles_in[:, cols]
            tile_ids[...] = jnp.zeros_like(tile_ids)
            for t in range(tiles):
                tile_ids[pl.ds(5 * t, 1), :] = nodes_in[pl.ds(t, 1), :]
                for a in range(4):
                    tile_ids[pl.ds(5 * t + 1 + a, 1), :] = facets_in[a, pl.ds(t, 1), :]
                live = jnp.where(t < count_in[0], 1.0, 0.0)
                weight_in[t] = mask_in[t].astype(F32) * live
            old_bodies = {}
            first_row = lax.broadcasted_iota(jnp.int32, (rows, LANES), 0) * LANES
            corner_low, corner_far = [], []
            for a in range(4):
                local = corner[pl.ds(a * rows, rows), :] - first_row
                corner_low.append(local & (LANES - 1))
                corner_far.append(local >= LANES)
                for i in range(rows):
                    hot = (sub == corner_low[a][i : i + 1]).astype(F32).astype(BF16)
                    win_hot[i, :, pl.ds(a * LANES, LANES)] = hot
            polar, azim = angle[pl.ds(0, rows), :], angle[pl.ds(rows, rows), :]

            def frame(polar, azim):
                cos_p, sin_p, cos_a, sin_a = jnp.cos(polar), jnp.sin(polar), jnp.cos(azim), jnp.sin(azim)
                return (cos_p * cos_a, cos_p * sin_a, -sin_p), (-sin_a, cos_a)

            volume = volume_in[...]
            mass = mass_in[...]
            gx = [grad[pl.ds(a * rows, rows), :] for a in range(4)]
            gy = [grad[pl.ds((4 + a) * rows, rows), :] for a in range(4)]
            own = (frame(polar, azim), volume, gx, gy, corner_low, corner_far)
            slots_high = tile_ids[...] // cap
            slots_low = tile_ids[...] % cap
            low_columns = jnp.transpose(slots_low)
            node_columns = jnp.transpose(send_in[0] & (LANES - 1))
            for g in range(group):
                column_buf[pl.ds(g * cap, cap), :] = jnp.broadcast_to(node_columns[:, g : g + 1], (cap, LANES))
            for b in range(5 * tiles):
                cols = pl.ds(b * LANES, LANES)
                for half in range(halves):
                    span = pl.ds(half * LANES, LANES)
                    hot = sub + half * LANES == slots_low[b : b + 1]
                    look_hot[span, cols] = hot.astype(F32).astype(F8)
                    hot = lane + half * LANES == low_columns[:, b : b + 1]
                    slot_hot[cols, span] = hot.astype(F32).astype(F8)
            for n, g in enumerate(arrival):
                hot = lane_tall == column_buf[pl.ds(pl.multiple_of(g * cap, cap), cap), :]
                node_hot[pl.ds(n * cap, cap), :] = hot.astype(F32).astype(F8)

        mine, landed = (send_buf, recv_buf) if step == 0 else (again_buf.at[step - 1], fresh_buf.at[step - 1])
        landed[my_place] = mine[my_place]
        depth = 6 if step == 0 else 3
        drain(landed.at[pl.ds(0, count), pl.ds(0, depth)], out_sem.at[step])
        table = []
        deep = 16 if step == 0 else 8
        for g in range(group):
            first, second = split(landed[g])
            if step == 0:
                table += [first, second]
            else:
                table.append(jnp.where(eight_wide < 4, first, jnp.roll(second, 4, axis=0)))
        table = jnp.concatenate(table, axis=0).astype(BF16)
        state = []
        for b in range(0, 5 * tiles, 2):
            looked = nn_dot(table, look_hot[:, pl.ds(b * LANES, 2 * LANES)])
            for side in range(2):
                high = jnp.broadcast_to(slots_high[b + side : b + side + 1], (8, LANES))
                block = looked[:, side * LANES : (side + 1) * LANES]
                first, second = block[:8], block[deep - 8 : deep]
                for g in range(1, group):
                    match = high == g
                    first = jnp.where(match, block[g * deep : g * deep + 8], first)
                    if step == 0:
                        second = jnp.where(match, block[g * deep + 8 : g * deep + 16], second)
                state.append(first + (second if step == 0 else jnp.roll(first, 4, axis=0)))
        slots = jnp.zeros((6 * group, cap), F32)
        for pair in range(tiles // 2):
            pair_tiles = (2 * pair, 2 * pair + 1)
            bodies = {}
            for t in pair_tiles:
                bodies[t, 0] = state[5 * t]
                bodies[t, 1] = 0.25 * sum(state[5 * t + 1 + a] for a in range(4))
            if step:
                for at in bodies:
                    moved = old_bodies[at] + TIME_STEP * jnp.roll(bodies[at], 3, axis=0)
                    bodies[at] = jnp.where(eight < 3, bodies[at], moved)
            if step + 1 < STEPS:
                old_bodies.update(bodies)
            columns = jnp.transpose(jnp.concatenate([bodies[t, 0] for t in pair_tiles], axis=0))
            for t in pair_tiles:
                mixes = [
                    jnp.where(
                        eight < 3, STIFFNESS * jnp.roll(bodies[t, s], 5, axis=0) - DAMPING * bodies[t, s], 0.0
                    )
                    for s in range(2)
                ]
                left_a, left_b = [
                    jnp.concatenate(two_parts(jnp.where(eight == 3, 1.0, mix)), axis=0) for mix in mixes
                ]
                dist = jnp.zeros((LANES, LANES), F32)
                for k in range(3, 6):
                    at = 8 * (t % 2) + k
                    gap = columns[:, at : at + 1] - bodies[t, 1][k : k + 1]
                    dist += gap * gap
                w1, w2 = two_parts(weight_in[t] * jnp.maximum(RADIUS_SQ - dist, 0.0))
                to_facet = nn_dot(
                    jnp.concatenate([left_a, left_a], axis=1), jnp.concatenate([w1, w2], axis=0)
                )
                to_node = nt_dot(
                    jnp.concatenate([left_b, left_b], axis=1), jnp.concatenate([w1, w2], axis=1)
                )
                to_facet = to_facet[:8] + to_facet[8:]
                to_node = to_node[:8] + to_node[8:]
                node_force = mixes[0] * to_node[3:4] - to_node
                facet_force = -0.25 * (to_facet - to_facet[3:4] * mixes[1])
                for force, blocks in ((node_force, [5 * t]), (facet_force, [5 * t + 1 + a for a in range(4)])):
                    matches = [group_iota == slots_high[b : b + 1] for b in blocks]
                    for part, value in enumerate(split(force)):
                        for k in range(3):
                            row = jnp.broadcast_to(value[k : k + 1], (group, LANES))
                            for b, match in zip(blocks, matches):
                                tile_lhs[pl.ds((part * 3 + k) * group, group), pl.ds(b * LANES, LANES)] = (
                                    jnp.where(match, row, 0.0).astype(BF16)
                                )
            at = pl.ds(pair * 10 * LANES, 10 * LANES)
            slots += nn_dot(tile_lhs[:, at], slot_hot[at, :])
        slots = slots[: 3 * group] + slots[3 * group :]
        for k in range(3):
            back_buf[step, :, k, :] = slots[k * group : (k + 1) * group]
        for j in range(count):
            group_copy(step, j, True).start()

        if step == 0:
            drain(force_rows.at[pl.ds(0, 18)], prev_sem.at[0])

            def whole(row):
                return jnp.broadcast_to(row, (8, LANES))

            prev_low, prev_far = [], []
            for a in range(4):
                local = corner_prev[pl.ds(a, 1), :] - (rows - 1) * LANES
                low = local & (LANES - 1)
                win_hot[rows, :, pl.ds(a * LANES, LANES)] = (sub == low).astype(F32).astype(BF16)
                prev_low.append(whole(low))
                prev_far.append(whole(local) >= LANES)
            prev = (
                frame(whole(angles_prev[pl.ds(0, 1), :]), whole(angles_prev[pl.ds(1, 1), :])),
                whole(volume_prev[...]),
                [whole(grad_prev[pl.ds(a, 1), :]) for a in range(4)],
                [whole(grad_prev[pl.ds(4 + a, 1), :]) for a in range(4)],
                prev_low, prev_far,
            )
            own_stress = [stress[pl.ds(k * rows, rows), :] for k in range(3)]
            prev_stress = [whole(stress_prev[pl.ds(k, 1), :]) for k in range(3)]

        def element_forces(batch, tension, near, far):
            (one, two), volume, gx, gy, low, beyond = batch
            corner_vel = [
                [
                    jnp.where(beyond[a], lane_take(far[k], low[a]), lane_take(near[k], low[a]))
                    for a in range(4)
                ]
                for k in range(3)
            ]
            xx = yy = xy = jnp.zeros(volume.shape, F32)
            for a in range(4):
                u = sum(one[k] * corner_vel[k][a] for k in range(3))
                w = sum(two[k] * corner_vel[k][a] for k in range(2))
                xx += gx[a] * u
                yy += gy[a] * w
                xy += gy[a] * u + gx[a] * w
            factor = TIME_STEP * YOUNG_MOD / (1.0 - POISSON * POISSON)
            sxx = tension[0] + factor * (xx + POISSON * yy)
            syy = tension[1] + factor * (POISSON * xx + yy)
            sxy = tension[2] + factor * 0.5 * (1.0 - POISSON) * xy
            hour = [
                HOURGLASS * volume
                * (corner_vel[k][0] - corner_vel[k][1] + corner_vel[k][2] - corner_vel[k][3])
                for k in range(3)
            ]
            forces = []
            for a in range(4):
                f1 = -volume * (gx[a] * sxx + gy[a] * sxy)
                f2 = -volume * (gy[a] * syy + gx[a] * sxy)
                parts = []
                for k in range(3):
                    force = one[k] * f1 - (1.0 if a % 2 == 0 else -1.0) * hour[k]
                    if k < 2:
                        force += two[k] * f2
                    first = force.astype(BF16).astype(F32)
                    parts.append((first, force - first))
                forces.append(parts)
            return [sxx, syy, sxy], forces

        drain(edge_recv.at[step], edge_sem.at[step])
        for k in range(3):
            vel[pl.ds(k * 2 * rows + rows, 1), :] = edge_recv[step, 0, pl.ds(k, 1), :]
        own_stress, forces = element_forces(
            own, own_stress,
            [velocity_rows(k) for k in range(3)],
            [vel[pl.ds(k * 2 * rows + 1, rows), :] for k in range(3)],
        )
        prev_stress, prev_forces = element_forces(
            prev, prev_stress,
            [whole(edge_recv[step, 1, pl.ds(k, 1), :]) for k in range(3)],
            [whole(vel[pl.ds(k * 2 * rows, 1), :]) for k in range(3)],
        )
        for a in range(4):
            for k in range(3):
                for part in range(2):
                    for side in range(2):
                        at = part * 8 + k * 2 + side
                        keep = corner_far[a] if side else jnp.logical_not(corner_far[a])
                        win_rows[a, pl.ds(at, rows, stride=16), :] = jnp.where(
                            keep, forces[a][k][part], 0.0
                        )
                        far_row = jnp.where(prev_far[a], prev_forces[a][k][part], 0.0)[:1]
                        win_rows[a, pl.ds(rows * 16 + at, 1), :] = far_row
        for i in range(rows + 1):
            left = jnp.concatenate(
                [win_rows[a, pl.ds(i * 16, 16), :].astype(BF16) for a in range(4)], axis=1
            )
            summed = nt_dot(left, win_hot[i])
            force_rows[pl.ds(i * 8, 8), :] = summed[:8] + summed[8:]
        internal = []
        for k in range(3):
            near = force_rows[pl.ds(k * 2, rows, stride=8), :]
            far = force_rows[pl.ds(k * 2 + 1, rows - 1, stride=8), :]
            edge_row = force_rows[pl.ds(rows * 8 + k * 2 + 1, 1), :]
            internal.append(near + jnp.concatenate([edge_row, far], axis=0))
        if step + 1 == STEPS:
            for k in range(3):
                for i in range(rows):
                    stress_out[pl.ds(k, 1), pl.ds(i * LANES, LANES)] = own_stress[k][i : i + 1]
        if step + 1 == STEPS:
            sent = count * halves * (6 + 3 * (STEPS - 1) + 3 * STEPS) + 6 * STEPS + 18
            drain(column_buf.at[pl.ds(0, sent)], send_sem.at[0])
        contact = jnp.zeros((3 * rows, LANES), F32)
        for begin in range(0, group, batch):
            answers = batch - 1 if begin == 0 else batch
            drain(answer_buf.at[step, pl.ds(0, answers), pl.ds(0, 3)], back_sem.at[step, int(begin > 0)])
            for n in range(begin, begin + batch):
                g = arrival[n]
                source = answer_buf if n else back_buf
                halved = split(source[step, g])
                for half in range(halves):
                    match = row_iota == slot_ids[g, pl.ds(half, 1), :]
                    at = pl.ds((n * halves + half) * LANES, LANES)
                    for part in range(2):
                        for k in range(3):
                            row = halved[part][k : k + 1, half * LANES : (half + 1) * LANES]
                            chosen = jnp.where(match, jnp.broadcast_to(row, match.shape), 0.0)
                            pairs[pl.ds((part * 3 + k) * rows, rows), at] = chosen.astype(BF16)
            at = pl.ds(begin * cap, batch * cap)
            summed = nn_dot(pairs[:, at], node_hot[at, :])
            contact += summed[: 3 * rows] + summed[3 * rows :]
        for k in range(3):
            fresh = velocity_rows(k) + TIME_STEP * (
                internal[k] + contact[k * rows : (k + 1) * rows]
            ) / mass
            vel[pl.ds(k * 2 * rows, rows), :] = fresh
            pos[pl.ds(k * rows, rows), :] = pos[pl.ds(k * rows, rows), :] + TIME_STEP * fresh

    for i in range(rows):
        cols = pl.ds(i * LANES, LANES)
        coords_out[:, cols] = pos[pl.ds(i, 3, stride=rows), :]
        velocity_out[:, cols] = vel[pl.ds(i, 3, stride=2 * rows), :]


def put_out(coords_in, velocity_in, stress_in, coords_out, velocity_out, stress_out, sems):
    pairs = ((coords_in, coords_out), (velocity_in, velocity_out), (stress_in, stress_out))
    copies = [pltpu.make_async_copy(src, dst, sems.at[n]) for n, (src, dst) in enumerate(pairs)]
    for copy in copies:
        copy.start()
    for copy in copies:
        copy.wait()


def per_device(
    sizes, coords, velocity, node_mass, corner_nodes, shape_grad, frame_angles, volume, stress,
    send_nodes, tile_count, tile_nodes, tile_facets, pair_mask,
):
    count = coords.shape[1]
    rows = count // LANES
    group = sizes[1] * sizes[2]
    cap = send_nodes.shape[2]
    tiles = tile_nodes.shape[0]
    vmem = pl.BlockSpec(memory_space=pltpu.VMEM)
    hbm = pl.BlockSpec(memory_space=pltpu.HBM)
    state = jax.ShapeDtypeStruct((3, count), F32)
    halves = cap // LANES
    arrays = (
        coords, velocity, node_mass.reshape(rows, LANES), corner_nodes, shape_grad, frame_angles,
        volume.reshape(rows, LANES), stress, send_nodes, tile_nodes, tile_facets, pair_mask,
    )
    arrays = tuple(pltpu.with_memory_space_constraint(a, pltpu.HBM) for a in arrays)
    dma = pltpu.SemaphoreType.DMA
    finals = pl.pallas_call(
        functools.partial(kernel, sizes),
        out_shape=(state, state, state),
        in_specs=[hbm] * 12 + [pl.BlockSpec(memory_space=pltpu.SMEM)],
        out_specs=(vmem, vmem, vmem),
        scratch_shapes=[pltpu.VMEM(a.shape, a.dtype) for a in arrays] + [
            dma((len(arrays),)),
            pltpu.VMEM((3 * rows, LANES), F32),
            pltpu.VMEM((6 * rows, LANES), F32),
            pltpu.VMEM((4 * rows, LANES), jnp.int32),
            pltpu.VMEM((8 * rows, LANES), F32),
            pltpu.VMEM((3 * rows, LANES), F32),
            pltpu.VMEM((2 * rows, LANES), F32),
            pltpu.VMEM((group, halves, LANES), jnp.int32),
            pltpu.VMEM((-(-5 * tiles // 8) * 8, LANES), jnp.int32),
            pltpu.VMEM((rows + 1, LANES, 4 * LANES), BF16),
            pltpu.VMEM((cap, 5 * tiles * LANES), F8),
            pltpu.VMEM((5 * tiles * LANES, cap), F8),
            pltpu.VMEM((group * cap, LANES), F8),
            pltpu.VMEM((4, 16 * (rows + 1), LANES), F32),
            pltpu.VMEM((8 * (rows + 1), LANES), F32),
            pltpu.VMEM((6 * group, 5 * tiles * LANES), BF16),
            pltpu.VMEM((6 * rows, group * cap), BF16),
            pltpu.VMEM((group * cap, LANES), jnp.int32),
            pltpu.VMEM((tiles, LANES, LANES), F32),
            pltpu.VMEM((group, 8, cap), F32),
            pltpu.VMEM((group, 8, cap), F32),
            pltpu.VMEM((STEPS - 1, group, 8, cap), F32),
            pltpu.VMEM((STEPS - 1, group, 8, cap), F32),
            pltpu.VMEM((STEPS, group, 4, cap), F32),
            pltpu.VMEM((STEPS, group, 4, cap), F32),
            pltpu.VMEM((STEPS - 1, 3, LANES), F32),
            pltpu.VMEM((STEPS - 1, 3, LANES), F32),
            pltpu.VMEM((STEPS, 2, 3, LANES), F32),
            pltpu.VMEM((4, LANES), jnp.int32),
            pltpu.VMEM((8, LANES), F32),
            pltpu.VMEM((2, LANES), F32),
            pltpu.VMEM((1, LANES), F32),
            pltpu.VMEM((3, LANES), F32),
            dma((1,)),
            dma((STEPS,)),
            dma((STEPS, 2)),
            dma((STEPS,)),
            dma((1,)),
        ],
        compiler_params=pltpu.CompilerParams(
            collective_id=0, has_side_effects=True, vmem_limit_bytes=24 * 1024 * 1024
        ),
    )(*arrays, tile_count)
    return pl.pallas_call(
        put_out,
        out_shape=(state, state, state),
        in_specs=[vmem] * 3,
        out_specs=(hbm, hbm, hbm),
        scratch_shapes=[dma((3,))],
        compiler_params=pltpu.CompilerParams(vmem_limit_bytes=1024 * 1024),
    )(*finals)


def solution(mesh):
    axes = ("len", "wid", "dep")
    flat, wide = P(axes), P(None, axes)
    sizes = tuple(mesh.shape[name] for name in axes)
    return jax.shard_map(
        functools.partial(per_device, sizes),
        mesh=mesh,
        in_specs=(
            wide, wide, flat, wide, wide, wide, flat, wide,
            P(axes, None, None), flat, P(axes, None), P(None, axes, None), P(axes, None, None),
        ),
        out_specs=(wide, wide, wide),
        check_vma=False,
    )
```

```python
import functools
import math

import jax
import jax.numpy as jnp
from jax import lax
from jax.experimental import pallas as pl
from jax.experimental.pallas import tpu as pltpu
from jax.sharding import PartitionSpec as P

STEPS = 2
TIME_STEP = 0.1
YOUNG_MOD = 1.0
POISSON = 0.3
HOURGLASS = 0.1
RADIUS_SQ = 1.0
STIFFNESS = 0.1
DAMPING = 0.05

LANES = 128
MESH = pl.DeviceIdType.MESH
F32 = jnp.float32
BF16 = jnp.bfloat16
F8 = jnp.float8_e4m3fn


def two_parts(values):
    first = values.astype(BF16)
    return first, (values - first.astype(F32)).astype(BF16)


def lane_take(table, low):
    return jnp.take_along_axis(table, low, axis=1, mode="promise_in_bounds")


def nt_dot(left, right):
    return lax.dot_general(left, right, (((1,), (1,)), ((), ())), preferred_element_type=F32)


def nn_dot(left, right):
    return lax.dot_general(left, right, (((1,), (0,)), ((), ())), preferred_element_type=F32)


def kernel(
    sizes,
    coords_hbm, velocity_hbm, mass_hbm, corner_hbm, grad_hbm, angles_hbm, volume_hbm, stress_hbm,
    send_hbm, nodes_hbm, facets_hbm, mask_hbm, count_in,
    coords_out, velocity_out, stress_out,
    coords_in, velocity_in, mass_in, corner_in, grad_in, angles_in, volume_in, stress_in,
    send_in, nodes_in, facets_in, mask_in, in_sem,
    pos, vel, corner, grad, stress, angle, slot_ids, tile_ids, win_hot, look_hot, slot_hot, node_hot,
    win_rows, force_rows, tile_lhs, pairs, column_buf, weight_in,
    send_buf, recv_buf, again_buf, fresh_buf, back_buf, answer_buf,
    first_buf, last_buf, edge_recv,
    corner_prev, grad_prev, angles_prev, volume_prev, stress_prev,
    send_sem, out_sem, back_sem, edge_sem,
):
    n_len, n_wid, n_dep = sizes
    group = n_wid * n_dep
    devices = n_len * group
    rows = coords_in.shape[1] // LANES
    cap = send_in.shape[2]
    halves = cap // LANES
    tiles = nodes_in.shape[0]
    my_len = lax.axis_index("len")
    my_wid = lax.axis_index("wid")
    my_dep = lax.axis_index("dep")
    my_place = my_wid * n_dep + my_dep
    my_id = my_len * group + my_place

    def by_id(p):
        return (p // group, (p % group) // n_dep, p % n_dep)

    upper = (2 * my_wid) // n_wid
    shifts = sorted(range(1, n_dep), key=lambda d: -min(d, n_dep - d))
    peers = []
    for r in range(n_wid):
        across = r + (1 - upper) * (n_wid - 1 - 2 * r)
        for shift in shifts:
            peers.append((across, lax.rem(my_dep + shift, n_dep)))
        if r < n_wid - 1:
            up = r + (r - my_wid + n_wid) // n_wid
            down = n_wid - 1 - r - (my_wid - (n_wid - 1 - r) + n_wid) // n_wid
            peers.append((upper * up + (1 - upper) * down, my_dep))
    places = [wid * n_dep + dep for wid, dep in peers]
    count = group - 1
    arrival = [my_place] + places[::-1]

    before = by_id(lax.rem(my_id + devices - 1, devices))
    after = by_id(lax.rem(my_id + 1, devices))

    loads = [
        pltpu.make_async_copy(src, dst, in_sem.at[min(n, 4)])
        for n, (src, dst) in enumerate((
            (send_hbm, send_in), (velocity_hbm, velocity_in), (coords_hbm, coords_in),
            (stress_hbm, stress_in), (corner_hbm, corner_in), (grad_hbm, grad_in),
            (angles_hbm, angles_in), (mass_hbm, mass_in), (volume_hbm, volume_in),
            (nodes_hbm, nodes_in), (facets_hbm, facets_in), (mask_hbm, mask_in),
        ))
    ]
    for load in loads[:3]:
        load.start()
    barrier = pltpu.get_barrier_semaphore()
    for wid, dep in peers:
        pl.semaphore_signal(barrier, inc=1, device_id=(my_len, wid, dep), device_id_type=MESH)
    pl.semaphore_signal(barrier, inc=1, device_id=before, device_id_type=MESH)
    pl.semaphore_signal(barrier, inc=1, device_id=after, device_id_type=MESH)
    for load in loads[3:]:
        load.start()
    for load in loads[:3]:
        load.wait()
    for i in range(rows):
        cols = pl.ds(i * LANES, LANES)
        pos[pl.ds(i, 3, stride=rows), :] = coords_in[:, cols]
        for k in range(3):
            vel[pl.ds(k * 2 * rows + i, 1), :] = velocity_in[pl.ds(k, 1), cols]

    def velocity_rows(k):
        return vel[pl.ds(k * 2 * rows, rows), :]

    def fill_edges(step):
        for k in range(3):
            first_buf[step - 1, pl.ds(k, 1), :] = vel[pl.ds(k * 2 * rows, 1), :]
            last_buf[step - 1, pl.ds(k, 1), :] = vel[pl.ds(k * 2 * rows + rows - 1, 1), :]

    segment = group // 2
    bases = [pl.multiple_of(side * segment, segment) for side in (1 - upper, upper)]

    def fill_slots(step, base):
        tables = [velocity_rows(k) for k in range(3)]
        if step == 0:
            tables += [pos[pl.ds(k * rows, rows), :] for k in range(3)]
        target = send_buf if step == 0 else again_buf.at[step - 1]
        for half in range(halves):
            cols = pl.ds(half * LANES, LANES)
            ids = send_in[0, pl.ds(base, segment), cols]
            low, high = ids & (LANES - 1), ids >> 7
            if step == 0:
                slot_ids[pl.ds(base, segment), half, :] = high
            for c, table in enumerate(tables):
                found = jnp.zeros(ids.shape, F32)
                for h in range(rows):
                    row = jnp.broadcast_to(table[h : h + 1], ids.shape)
                    found = jnp.where(high == h, lane_take(row, low), found)
                target[pl.ds(base, segment), c, cols] = found

    def remote(src, dst, recv_sem, target):
        return pltpu.make_async_remote_copy(
            src_ref=src, dst_ref=dst, send_sem=send_sem.at[0], recv_sem=recv_sem,
            device_id=target, device_id_type=MESH,
        )

    def drain(ref, sem):
        pltpu.make_async_copy(ref, ref, sem).wait()

    final = pl.ds((rows - 1) * LANES, LANES)

    def edge_copies(step):
        if step == 0:
            first, last = velocity_in.at[:, pl.ds(0, LANES)], velocity_in.at[:, final]
        else:
            first, last = first_buf.at[step - 1], last_buf.at[step - 1]
        return (
            remote(first, edge_recv.at[step, 0], edge_sem.at[step], before),
            remote(last, edge_recv.at[step, 1], edge_sem.at[step], after),
        )

    def prev_copies():
        pairs = (
            (corner_in.at[:, final], corner_prev), (grad_in.at[:, final], grad_prev),
            (angles_in.at[:, final], angles_prev), (stress_in.at[:, final], stress_prev),
            (volume_in.at[pl.ds(rows - 1, 1), :], volume_prev),
        )
        return [
            remote(src, dst, edge_sem.at[STEPS], after) for src, dst in pairs
        ]

    far_count = n_dep * (n_wid // 2)

    def group_copy(step, j, back):
        wid, dep = peers[j]
        if back:
            src, dst, depth, sem = back_buf.at[step], answer_buf.at[step], 3, back_sem.at[step, int(j < far_count)]
        elif step == 0:
            src, dst, depth, sem = send_buf, recv_buf, 6, out_sem.at[step, int(j < far_count)]
        else:
            src, dst, depth, sem = again_buf.at[step - 1], fresh_buf.at[step - 1], 3, out_sem.at[step, int(j < far_count)]
        return remote(
            src.at[places[j], pl.ds(0, depth)], dst.at[my_place, pl.ds(0, depth)], sem, (my_len, wid, dep)
        )

    batch = count + 1 - far_count
    parts = ((bases[0], range(far_count)), (bases[1], range(far_count, count)))

    fill_slots(0, bases[0])
    pl.semaphore_wait(barrier, group + 1)

    sub = lax.broadcasted_iota(jnp.int32, (LANES, LANES), 0)
    lane = lax.broadcasted_iota(jnp.int32, (LANES, LANES), 1)
    lane_tall = lax.broadcasted_iota(jnp.int32, (cap, LANES), 1)
    eight = lax.broadcasted_iota(jnp.int32, (8, LANES), 0)
    row_iota = lax.broadcasted_iota(jnp.int32, (rows, LANES), 0)
    eight_wide = lax.broadcasted_iota(jnp.int32, (8, cap), 0)
    group_iota = lax.broadcasted_iota(jnp.int32, (group, LANES), 0)

    def split(values):
        first = values.astype(BF16).astype(F32)
        return first, values - first

    for step in range(STEPS):
        for base, span in parts:
            if step or base is not bases[0]:
                fill_slots(step, base)
            for j in span:
                group_copy(step, j, False).start()
        if step:
            fill_edges(step)
        for copy in edge_copies(step):
            copy.start()

        if step == 0:
            loads[3].wait()
            words = sum(math.prod(dst.shape) for dst in (
                corner_in, grad_in, angles_in, mass_in, volume_in, nodes_in, facets_in, mask_in,
            ))
            drain(column_buf.at[pl.ds(0, words // LANES)], in_sem.at[4])
            for copy in prev_copies():
                copy.start()
            for i in range(rows):
                cols = pl.ds(i * LANES, LANES)
                stress[pl.ds(i, 3, stride=rows), :] = stress_in[:, cols]
                corner[pl.ds(i, 4, stride=rows), :] = corner_in[:, cols]
                grad[pl.ds(i, 8, stride=rows), :] = grad_in[:, cols]
                angle[pl.ds(i, 2, stride=rows), :] = angles_in[:, cols]
            tile_ids[...] = jnp.zeros_like(tile_ids)
            for t in range(tiles):
                tile_ids[pl.ds(5 * t, 1), :] = nodes_in[pl.ds(t, 1), :]
                for a in range(4):
                    tile_ids[pl.ds(5 * t + 1 + a, 1), :] = facets_in[a, pl.ds(t, 1), :]
                live = jnp.where(t < count_in[0], 1.0, 0.0)
                weight_in[t] = mask_in[t].astype(F32) * live
            old_bodies = {}
            first_row = lax.broadcasted_iota(jnp.int32, (rows, LANES), 0) * LANES
            corner_low, corner_far = [], []
            for a in range(4):
                local = corner[pl.ds(a * rows, rows), :] - first_row
                corner_low.append(local & (LANES - 1))
                corner_far.append(local >= LANES)
                for i in range(rows):
                    hot = (sub == corner_low[a][i : i + 1]).astype(F32).astype(BF16)
                    win_hot[i, :, pl.ds(a * LANES, LANES)] = hot
            polar, azim = angle[pl.ds(0, rows), :], angle[pl.ds(rows, rows), :]

            def frame(polar, azim):
                cos_p, sin_p, cos_a, sin_a = jnp.cos(polar), jnp.sin(polar), jnp.cos(azim), jnp.sin(azim)
                return (cos_p * cos_a, cos_p * sin_a, -sin_p), (-sin_a, cos_a)

            volume = volume_in[...]
            pace = TIME_STEP / mass_in[...]
            gx = [grad[pl.ds(a * rows, rows), :] for a in range(4)]
            gy = [grad[pl.ds((4 + a) * rows, rows), :] for a in range(4)]
            own = (frame(polar, azim), volume, gx, gy, corner_low, corner_far)
            slots_high = tile_ids[...] // cap
            slots_low = tile_ids[...] % cap
            low_columns = jnp.transpose(slots_low)
            node_columns = jnp.transpose(send_in[0] & (LANES - 1))
            for g in range(group):
                column_buf[pl.ds(g * cap, cap), :] = jnp.broadcast_to(node_columns[:, g : g + 1], (cap, LANES))
            for b in range(5 * tiles):
                cols = pl.ds(b * LANES, LANES)
                for half in range(halves):
                    span = pl.ds(half * LANES, LANES)
                    hot = sub + half * LANES == slots_low[b : b + 1]
                    look_hot[span, cols] = hot.astype(F32).astype(F8)
                    hot = lane + half * LANES == low_columns[:, b : b + 1]
                    slot_hot[cols, span] = hot.astype(F32).astype(F8)
            for n, g in enumerate(arrival):
                hot = lane_tall == column_buf[pl.ds(pl.multiple_of(g * cap, cap), cap), :]
                node_hot[pl.ds(n * cap, cap), :] = hot.astype(F32).astype(F8)

        mine, landed = (send_buf, recv_buf) if step == 0 else (again_buf.at[step - 1], fresh_buf.at[step - 1])
        landed[my_place] = mine[my_place]
        depth = 6 if step == 0 else 3
        deep = 16 if step == 0 else 8
        taken = [[jnp.zeros((8, LANES), F32)] * (deep // 8) for b in range(5 * tiles)]
        for far, base in ((0, bases[1]), (1, bases[0])):
            landing = far_count if far else count - far_count
            drain(landed.at[pl.ds(0, landing), pl.ds(0, depth)], out_sem.at[step, far])
            table = []
            for g in range(segment):
                first, second = split(landed[base + g])
                if step == 0:
                    table += [first, second]
                else:
                    table.append(jnp.where(eight_wide < 4, first, jnp.roll(second, 4, axis=0)))
            table = jnp.concatenate(table, axis=0).astype(BF16)
            for b in range(0, 5 * tiles, 2):
                looked = nn_dot(table, look_hot[:, pl.ds(b * LANES, 2 * LANES)])
                for side in range(2):
                    high = jnp.broadcast_to(slots_high[b + side : b + side + 1] - base, (8, LANES))
                    block = looked[:, side * LANES : (side + 1) * LANES]
                    for g in range(segment):
                        match = high == g
                        taken[b + side] = [
                            jnp.where(match, block[g * deep + 8 * p : g * deep + 8 * p + 8], old)
                            for p, old in enumerate(taken[b + side])
                        ]
        state = [t[0] + (t[1] if step == 0 else jnp.roll(t[0], 4, axis=0)) for t in taken]
        slots = jnp.zeros((6 * group, cap), F32)
        for pair in range(tiles // 2):
            pair_tiles = (2 * pair, 2 * pair + 1)
            bodies = {}
            for t in pair_tiles:
                bodies[t, 0] = state[5 * t]
                bodies[t, 1] = 0.25 * sum(state[5 * t + 1 + a] for a in range(4))
            if step:
                for at in bodies:
                    moved = old_bodies[at] + TIME_STEP * jnp.roll(bodies[at], 3, axis=0)
                    bodies[at] = jnp.where(eight < 3, bodies[at], moved)
            if step + 1 < STEPS:
                old_bodies.update(bodies)
            tall, across_rows = [], [[] for _ in range(6)]
            for t in pair_tiles:
                high_part, rest = split(bodies[t, 0])
                mid_part, low_part = split(rest)
                tall.append(jnp.where(
                    eight % 4 == 3, 1.0,
                    jnp.where(eight < 3, jnp.roll(high_part, 5, axis=0), jnp.roll(mid_part, 1, axis=0)),
                ))
                tall.append(jnp.where(eight < 3, jnp.roll(low_part, 5, axis=0), jnp.where(eight == 3, 1.0, 0.0)))
                high_part, rest = split(-bodies[t, 1])
                mid_part, low_part = split(rest)
                for k in range(3):
                    unit = jnp.where(eight % 4 == k, 1.0, 0.0)
                    spread = [jnp.broadcast_to(p[3 + k : 4 + k], (8, LANES)) for p in (high_part, mid_part, low_part)]
                    block = [
                        jnp.where(eight == 3, spread[0], jnp.where(eight == 7, spread[1], unit)),
                        jnp.where(eight == 3, spread[2], jnp.where(eight < 3, unit, 0.0)),
                    ]
                    none = [jnp.zeros((8, LANES), F32)] * 2
                    whole_block = block + none if t % 2 == 0 else none + block
                    across_rows[3 * (t % 2) + k] = jnp.concatenate(whole_block, axis=0)
            gaps = nn_dot(
                jnp.transpose(jnp.concatenate(tall, axis=0)).astype(BF16),
                jnp.concatenate(across_rows, axis=1).astype(BF16),
            )
            for t in pair_tiles:
                mixes = [
                    jnp.where(
                        eight < 3, STIFFNESS * jnp.roll(bodies[t, s], 5, axis=0) - DAMPING * bodies[t, s], 0.0
                    )
                    for s in range(2)
                ]
                left_a, left_b = [
                    jnp.concatenate(two_parts(jnp.where(eight == 3, 1.0, mix)), axis=0) for mix in mixes
                ]
                dist = jnp.zeros((LANES, LANES), F32)
                for k in range(3):
                    at = (3 * (t % 2) + k) * LANES
                    gap = gaps[:, at : at + LANES]
                    dist += gap * gap
                w1, w2 = two_parts(weight_in[t] * jnp.maximum(RADIUS_SQ - dist, 0.0))
                to_facet = nn_dot(
                    jnp.concatenate([left_a, left_a], axis=1), jnp.concatenate([w1, w2], axis=0)
                )
                to_node = nt_dot(
                    jnp.concatenate([left_b, left_b], axis=1), jnp.concatenate([w1, w2], axis=1)
                )
                to_facet = to_facet[:8] + to_facet[8:]
                to_node = to_node[:8] + to_node[8:]
                node_force = mixes[0] * to_node[3:4] - to_node
                facet_force = -0.25 * (to_facet - to_facet[3:4] * mixes[1])
                for force, blocks in ((node_force, [5 * t]), (facet_force, [5 * t + 1 + a for a in range(4)])):
                    matches = [group_iota == slots_high[b : b + 1] for b in blocks]
                    for part, value in enumerate(split(force)):
                        for k in range(3):
                            row = jnp.broadcast_to(value[k : k + 1], (group, LANES))
                            for b, match in zip(blocks, matches):
                                tile_lhs[pl.ds((part * 3 + k) * group, group), pl.ds(b * LANES, LANES)] = (
                                    jnp.where(match, row, 0.0).astype(BF16)
                                )
            at = pl.ds(pair * 10 * LANES, 10 * LANES)
            slots += nn_dot(tile_lhs[:, at], slot_hot[at, :])
        slots = slots[: 3 * group] + slots[3 * group :]
        for k in range(3):
            back_buf[step, :, k, :] = slots[k * group : (k + 1) * group]
        for j in range(count):
            group_copy(step, j, True).start()

        if step == 0:
            drain(force_rows.at[pl.ds(0, 18)], edge_sem.at[STEPS])

            def whole(row):
                return jnp.broadcast_to(row, (8, LANES))

            prev_low, prev_far = [], []
            for a in range(4):
                local = corner_prev[pl.ds(a, 1), :] - (rows - 1) * LANES
                low = local & (LANES - 1)
                win_hot[rows, :, pl.ds(a * LANES, LANES)] = (sub == low).astype(F32).astype(BF16)
                prev_low.append(whole(low))
                prev_far.append(whole(local) >= LANES)
            prev = (
                frame(whole(angles_prev[pl.ds(0, 1), :]), whole(angles_prev[pl.ds(1, 1), :])),
                whole(volume_prev[...]),
                [whole(grad_prev[pl.ds(a, 1), :]) for a in range(4)],
                [whole(grad_prev[pl.ds(4 + a, 1), :]) for a in range(4)],
                prev_low, prev_far,
            )
            own_stress = [stress[pl.ds(k * rows, rows), :] for k in range(3)]
            prev_stress = [whole(stress_prev[pl.ds(k, 1), :]) for k in range(3)]

        def element_forces(batch, tension, near, far):
            (one, two), volume, gx, gy, low, beyond = batch
            corner_vel = [
                [
                    jnp.where(beyond[a], lane_take(far[k], low[a]), lane_take(near[k], low[a]))
                    for a in range(4)
                ]
                for k in range(3)
            ]
            xx = yy = xy = jnp.zeros(volume.shape, F32)
            for a in range(4):
                u = sum(one[k] * corner_vel[k][a] for k in range(3))
                w = sum(two[k] * corner_vel[k][a] for k in range(2))
                xx += gx[a] * u
                yy += gy[a] * w
                xy += gy[a] * u + gx[a] * w
            factor = TIME_STEP * YOUNG_MOD / (1.0 - POISSON * POISSON)
            sxx = tension[0] + factor * (xx + POISSON * yy)
            syy = tension[1] + factor * (POISSON * xx + yy)
            sxy = tension[2] + factor * 0.5 * (1.0 - POISSON) * xy
            hour = [
                HOURGLASS * volume
                * (corner_vel[k][0] - corner_vel[k][1] + corner_vel[k][2] - corner_vel[k][3])
                for k in range(3)
            ]
            forces = []
            for a in range(4):
                f1 = -volume * (gx[a] * sxx + gy[a] * sxy)
                f2 = -volume * (gy[a] * syy + gx[a] * sxy)
                parts = []
                for k in range(3):
                    force = one[k] * f1 - (1.0 if a % 2 == 0 else -1.0) * hour[k]
                    if k < 2:
                        force += two[k] * f2
                    first = force.astype(BF16).astype(F32)
                    parts.append((first, force - first))
                forces.append(parts)
            return [sxx, syy, sxy], forces

        drain(edge_recv.at[step], edge_sem.at[step])
        for k in range(3):
            vel[pl.ds(k * 2 * rows + rows, 1), :] = edge_recv[step, 0, pl.ds(k, 1), :]
        own_stress, forces = element_forces(
            own, own_stress,
            [velocity_rows(k) for k in range(3)],
            [vel[pl.ds(k * 2 * rows + 1, rows), :] for k in range(3)],
        )
        prev_stress, prev_forces = element_forces(
            prev, prev_stress,
            [whole(edge_recv[step, 1, pl.ds(k, 1), :]) for k in range(3)],
            [whole(vel[pl.ds(k * 2 * rows, 1), :]) for k in range(3)],
        )
        for a in range(4):
            for k in range(3):
                for part in range(2):
                    for side in range(2):
                        at = part * 8 + k * 2 + side
                        keep = corner_far[a] if side else jnp.logical_not(corner_far[a])
                        win_rows[a, pl.ds(at, rows, stride=16), :] = jnp.where(
                            keep, forces[a][k][part], 0.0
                        )
                        far_row = jnp.where(prev_far[a], prev_forces[a][k][part], 0.0)[:1]
                        win_rows[a, pl.ds(rows * 16 + at, 1), :] = far_row
        for i in range(rows + 1):
            left = jnp.concatenate(
                [win_rows[a, pl.ds(i * 16, 16), :].astype(BF16) for a in range(4)], axis=1
            )
            summed = nt_dot(left, win_hot[i])
            force_rows[pl.ds(i * 8, 8), :] = summed[:8] + summed[8:]
        internal = []
        for k in range(3):
            near = force_rows[pl.ds(k * 2, rows, stride=8), :]
            far = force_rows[pl.ds(k * 2 + 1, rows - 1, stride=8), :]
            edge_row = force_rows[pl.ds(rows * 8 + k * 2 + 1, 1), :]
            internal.append(near + jnp.concatenate([edge_row, far], axis=0))
        if step + 1 == STEPS:
            for k in range(3):
                for i in range(rows):
                    stress_out[pl.ds(k, 1), pl.ds(i * LANES, LANES)] = own_stress[k][i : i + 1]
        if step + 1 == STEPS:
            sent = count * halves * (6 + 3 * (STEPS - 1) + 3 * STEPS) + 6 * STEPS + 18
            drain(column_buf.at[pl.ds(0, sent)], send_sem.at[0])
        contact = jnp.zeros((3 * rows, LANES), F32)
        for begin in range(0, group, batch):
            answers = batch - 1 if begin == 0 else batch
            drain(answer_buf.at[step, pl.ds(0, answers), pl.ds(0, 3)], back_sem.at[step, int(begin > 0)])
            for n in range(begin, begin + batch):
                g = arrival[n]
                source = answer_buf if n else back_buf
                halved = split(source[step, g])
                for half in range(halves):
                    match = row_iota == slot_ids[g, pl.ds(half, 1), :]
                    at = pl.ds((n * halves + half) * LANES, LANES)
                    for part in range(2):
                        for k in range(3):
                            row = halved[part][k : k + 1, half * LANES : (half + 1) * LANES]
                            chosen = jnp.where(match, jnp.broadcast_to(row, match.shape), 0.0)
                            pairs[pl.ds((part * 3 + k) * rows, rows), at] = chosen.astype(BF16)
            at = pl.ds(begin * cap, batch * cap)
            summed = nn_dot(pairs[:, at], node_hot[at, :])
            contact += summed[: 3 * rows] + summed[3 * rows :]
        for k in range(3):
            fresh = velocity_rows(k) + pace * (internal[k] + contact[k * rows : (k + 1) * rows])
            vel[pl.ds(k * 2 * rows, rows), :] = fresh
            pos[pl.ds(k * rows, rows), :] = pos[pl.ds(k * rows, rows), :] + TIME_STEP * fresh

    for i in range(rows):
        cols = pl.ds(i * LANES, LANES)
        coords_out[:, cols] = pos[pl.ds(i, 3, stride=rows), :]
        velocity_out[:, cols] = vel[pl.ds(i, 3, stride=2 * rows), :]


def put_out(coords_in, velocity_in, stress_in, coords_out, velocity_out, stress_out, sems):
    pairs = ((coords_in, coords_out), (velocity_in, velocity_out), (stress_in, stress_out))
    copies = [pltpu.make_async_copy(src, dst, sems.at[n]) for n, (src, dst) in enumerate(pairs)]
    for copy in copies:
        copy.start()
    for copy in copies:
        copy.wait()


def per_device(
    sizes, coords, velocity, node_mass, corner_nodes, shape_grad, frame_angles, volume, stress,
    send_nodes, tile_count, tile_nodes, tile_facets, pair_mask,
):
    count = coords.shape[1]
    rows = count // LANES
    group = sizes[1] * sizes[2]
    cap = send_nodes.shape[2]
    tiles = tile_nodes.shape[0]
    vmem = pl.BlockSpec(memory_space=pltpu.VMEM)
    hbm = pl.BlockSpec(memory_space=pltpu.HBM)
    state = jax.ShapeDtypeStruct((3, count), F32)
    halves = cap // LANES
    arrays = (
        coords, velocity, node_mass.reshape(rows, LANES), corner_nodes, shape_grad, frame_angles,
        volume.reshape(rows, LANES), stress, send_nodes, tile_nodes, tile_facets, pair_mask,
    )
    arrays = tuple(pltpu.with_memory_space_constraint(a, pltpu.HBM) for a in arrays)
    dma = pltpu.SemaphoreType.DMA
    finals = pl.pallas_call(
        functools.partial(kernel, sizes),
        out_shape=(state, state, state),
        in_specs=[hbm] * 12 + [pl.BlockSpec(memory_space=pltpu.SMEM)],
        out_specs=(vmem, vmem, vmem),
        scratch_shapes=[pltpu.VMEM(a.shape, a.dtype) for a in arrays] + [
            dma((5,)),
            pltpu.VMEM((3 * rows, LANES), F32),
            pltpu.VMEM((6 * rows, LANES), F32),
            pltpu.VMEM((4 * rows, LANES), jnp.int32),
            pltpu.VMEM((8 * rows, LANES), F32),
            pltpu.VMEM((3 * rows, LANES), F32),
            pltpu.VMEM((2 * rows, LANES), F32),
            pltpu.VMEM((group, halves, LANES), jnp.int32),
            pltpu.VMEM((-(-5 * tiles // 8) * 8, LANES), jnp.int32),
            pltpu.VMEM((rows + 1, LANES, 4 * LANES), BF16),
            pltpu.VMEM((cap, 5 * tiles * LANES), F8),
            pltpu.VMEM((5 * tiles * LANES, cap), F8),
            pltpu.VMEM((group * cap, LANES), F8),
            pltpu.VMEM((4, 16 * (rows + 1), LANES), F32),
            pltpu.VMEM((8 * (rows + 1), LANES), F32),
            pltpu.VMEM((6 * group, 5 * tiles * LANES), BF16),
            pltpu.VMEM((6 * rows, group * cap), BF16),
            pltpu.VMEM((group * cap, LANES), jnp.int32),
            pltpu.VMEM((tiles, LANES, LANES), F32),
            pltpu.VMEM((group, 8, cap), F32),
            pltpu.VMEM((group, 8, cap), F32),
            pltpu.VMEM((STEPS - 1, group, 8, cap), F32),
            pltpu.VMEM((STEPS - 1, group, 8, cap), F32),
            pltpu.VMEM((STEPS, group, 4, cap), F32),
            pltpu.VMEM((STEPS, group, 4, cap), F32),
            pltpu.VMEM((STEPS - 1, 3, LANES), F32),
            pltpu.VMEM((STEPS - 1, 3, LANES), F32),
            pltpu.VMEM((STEPS, 2, 3, LANES), F32),
            pltpu.VMEM((4, LANES), jnp.int32),
            pltpu.VMEM((8, LANES), F32),
            pltpu.VMEM((2, LANES), F32),
            pltpu.VMEM((1, LANES), F32),
            pltpu.VMEM((3, LANES), F32),
            dma((1,)),
            dma((STEPS, 2)),
            dma((STEPS, 2)),
            dma((STEPS + 1,)),
        ],
        compiler_params=pltpu.CompilerParams(
            collective_id=0, has_side_effects=True, vmem_limit_bytes=24 * 1024 * 1024
        ),
    )(*arrays, tile_count)
    return pl.pallas_call(
        put_out,
        out_shape=(state, state, state),
        in_specs=[vmem] * 3,
        out_specs=(hbm, hbm, hbm),
        scratch_shapes=[dma((3,))],
        compiler_params=pltpu.CompilerParams(vmem_limit_bytes=1024 * 1024),
    )(*finals)


def solution(mesh):
    axes = ("len", "wid", "dep")
    flat, wide = P(axes), P(None, axes)
    sizes = tuple(mesh.shape[name] for name in axes)
    return jax.shard_map(
        functools.partial(per_device, sizes),
        mesh=mesh,
        in_specs=(
            wide, wide, flat, wide, wide, wide, flat, wide,
            P(axes, None, None), flat, P(axes, None), P(None, axes, None), P(axes, None, None),
        ),
        out_specs=(wide, wide, wide),
        check_vma=False,
    )
```

```python
import functools
import math

import jax
import jax.numpy as jnp
from jax import lax
from jax.experimental import pallas as pl
from jax.experimental.pallas import tpu as pltpu
from jax.sharding import PartitionSpec as P

STEPS = 2
TIME_STEP = 0.1
YOUNG_MOD = 1.0
POISSON = 0.3
HOURGLASS = 0.1
RADIUS_SQ = 1.0
STIFFNESS = 0.1
DAMPING = 0.05

LANES = 128
MESH = pl.DeviceIdType.MESH
F32 = jnp.float32
BF16 = jnp.bfloat16
F8 = jnp.float8_e4m3fn


def two_parts(values):
    first = values.astype(BF16)
    return first, (values - first.astype(F32)).astype(BF16)


def lane_take(table, low):
    return jnp.take_along_axis(table, low, axis=1, mode="promise_in_bounds")


def nt_dot(left, right):
    return lax.dot_general(left, right, (((1,), (1,)), ((), ())), preferred_element_type=F32)


def nn_dot(left, right):
    return lax.dot_general(left, right, (((1,), (0,)), ((), ())), preferred_element_type=F32)


def kernel(
    sizes,
    coords_hbm, velocity_hbm, mass_hbm, corner_hbm, grad_hbm, angles_hbm, volume_hbm, stress_hbm,
    send_hbm, nodes_hbm, facets_hbm, mask_hbm, count_in,
    coords_out, velocity_out, stress_out,
    coords_in, velocity_in, mass_in, corner_in, grad_in, angles_in, volume_in, stress_in,
    send_in, nodes_in, facets_in, mask_in, in_sem,
    pos, vel, corner, grad, stress, angle, slot_ids, tile_ids, win_hot, look_hot, slot_hot, node_hot,
    win_rows, force_rows, tile_lhs, pairs, column_buf, weight_in,
    send_buf, recv_buf, again_buf, fresh_buf, back_buf, answer_buf,
    first_buf, last_buf, edge_recv,
    corner_prev, grad_prev, angles_prev, volume_prev, stress_prev,
    send_sem, out_sem, back_sem, edge_sem,
):
    n_len, n_wid, n_dep = sizes
    group = n_wid * n_dep
    devices = n_len * group
    rows = coords_in.shape[1] // LANES
    cap = send_in.shape[2]
    halves = cap // LANES
    tiles = nodes_in.shape[0]
    my_len = lax.axis_index("len")
    my_wid = lax.axis_index("wid")
    my_dep = lax.axis_index("dep")
    my_place = my_wid * n_dep + my_dep
    my_id = my_len * group + my_place

    def by_id(p):
        return (p // group, (p % group) // n_dep, p % n_dep)

    upper = (2 * my_wid) // n_wid
    shifts = sorted(range(1, n_dep), key=lambda d: -min(d, n_dep - d))
    peers = []
    for r in range(n_wid):
        across = r + (1 - upper) * (n_wid - 1 - 2 * r)
        for shift in shifts:
            peers.append((across, lax.rem(my_dep + shift, n_dep)))
        if r < n_wid - 1:
            up = r + (r - my_wid + n_wid) // n_wid
            down = n_wid - 1 - r - (my_wid - (n_wid - 1 - r) + n_wid) // n_wid
            peers.append((upper * up + (1 - upper) * down, my_dep))
    places = [wid * n_dep + dep for wid, dep in peers]
    count = group - 1
    arrival = [my_place] + places[::-1]

    before = by_id(lax.rem(my_id + devices - 1, devices))
    after = by_id(lax.rem(my_id + 1, devices))

    loads = [
        pltpu.make_async_copy(src, dst, in_sem.at[min(n, 4)])
        for n, (src, dst) in enumerate((
            (send_hbm, send_in), (velocity_hbm, velocity_in), (coords_hbm, coords_in),
            (stress_hbm, stress_in), (corner_hbm, corner_in), (grad_hbm, grad_in),
            (angles_hbm, angles_in), (mass_hbm, mass_in), (volume_hbm, volume_in),
            (nodes_hbm, nodes_in), (facets_hbm, facets_in), (mask_hbm, mask_in),
        ))
    ]
    for load in loads[:3]:
        load.start()
    barrier = pltpu.get_barrier_semaphore()
    for wid, dep in peers:
        pl.semaphore_signal(barrier, inc=1, device_id=(my_len, wid, dep), device_id_type=MESH)
    pl.semaphore_signal(barrier, inc=1, device_id=before, device_id_type=MESH)
    pl.semaphore_signal(barrier, inc=1, device_id=after, device_id_type=MESH)
    for load in loads[3:]:
        load.start()
    for load in loads[:3]:
        load.wait()
    for i in range(rows):
        cols = pl.ds(i * LANES, LANES)
        pos[pl.ds(i, 3, stride=rows), :] = coords_in[:, cols]
        for k in range(3):
            vel[pl.ds(k * 2 * rows + i, 1), :] = velocity_in[pl.ds(k, 1), cols]

    def velocity_rows(k):
        return vel[pl.ds(k * 2 * rows, rows), :]

    def fill_edges(step):
        for k in range(3):
            first_buf[step - 1, pl.ds(k, 1), :] = vel[pl.ds(k * 2 * rows, 1), :]
            last_buf[step - 1, pl.ds(k, 1), :] = vel[pl.ds(k * 2 * rows + rows - 1, 1), :]

    segment = group // 2
    bases = [pl.multiple_of(side * segment, segment) for side in (1 - upper, upper)]

    def fill_slots(step, base):
        tables = [velocity_rows(k) for k in range(3)]
        if step == 0:
            tables += [pos[pl.ds(k * rows, rows), :] for k in range(3)]
        target = send_buf if step == 0 else again_buf.at[step - 1]
        for half in range(halves):
            cols = pl.ds(half * LANES, LANES)
            ids = send_in[0, pl.ds(base, segment), cols]
            low, high = ids & (LANES - 1), ids >> 7
            if step == 0:
                slot_ids[pl.ds(base, segment), half, :] = high
            for c, table in enumerate(tables):
                found = jnp.zeros(ids.shape, F32)
                for h in range(rows):
                    row = jnp.broadcast_to(table[h : h + 1], ids.shape)
                    found = jnp.where(high == h, lane_take(row, low), found)
                target[pl.ds(base, segment), c, cols] = found

    def remote(src, dst, recv_sem, target):
        return pltpu.make_async_remote_copy(
            src_ref=src, dst_ref=dst, send_sem=send_sem.at[0], recv_sem=recv_sem,
            device_id=target, device_id_type=MESH,
        )

    def drain(ref, sem):
        pltpu.make_async_copy(ref, ref, sem).wait()

    final = pl.ds((rows - 1) * LANES, LANES)

    def edge_copies(step):
        if step == 0:
            first, last = velocity_in.at[:, pl.ds(0, LANES)], velocity_in.at[:, final]
        else:
            first, last = first_buf.at[step - 1], last_buf.at[step - 1]
        return (
            remote(first, edge_recv.at[step, 0], edge_sem.at[step], before),
            remote(last, edge_recv.at[step, 1], edge_sem.at[step], after),
        )

    def prev_copies():
        pairs = (
            (corner_in.at[:, final], corner_prev), (grad_in.at[:, final], grad_prev),
            (angles_in.at[:, final], angles_prev), (stress_in.at[:, final], stress_prev),
            (volume_in.at[pl.ds(rows - 1, 1), :], volume_prev),
        )
        return [
            remote(src, dst, edge_sem.at[STEPS], after) for src, dst in pairs
        ]

    far_count = n_dep * (n_wid // 2)

    def group_copy(step, j, back):
        wid, dep = peers[j]
        if back:
            src, dst, depth, sem = back_buf.at[step], answer_buf.at[step], 3, back_sem.at[step, int(j < far_count)]
        elif step == 0:
            src, dst, depth, sem = send_buf, recv_buf, 6, out_sem.at[step, int(j < far_count)]
        else:
            src, dst, depth, sem = again_buf.at[step - 1], fresh_buf.at[step - 1], 3, out_sem.at[step, int(j < far_count)]
        return remote(
            src.at[places[j], pl.ds(0, depth)], dst.at[my_place, pl.ds(0, depth)], sem, (my_len, wid, dep)
        )

    batch = count + 1 - far_count
    parts = ((bases[0], range(far_count)), (bases[1], range(far_count, count)))

    fill_slots(0, bases[0])
    pl.semaphore_wait(barrier, group + 1)

    sub = lax.broadcasted_iota(jnp.int32, (LANES, LANES), 0)
    lane = lax.broadcasted_iota(jnp.int32, (LANES, LANES), 1)
    lane_tall = lax.broadcasted_iota(jnp.int32, (cap, LANES), 1)
    eight = lax.broadcasted_iota(jnp.int32, (8, LANES), 0)
    row_iota = lax.broadcasted_iota(jnp.int32, (rows, LANES), 0)
    eight_wide = lax.broadcasted_iota(jnp.int32, (8, cap), 0)
    group_iota = lax.broadcasted_iota(jnp.int32, (group, LANES), 0)

    def split(values):
        first = values.astype(BF16).astype(F32)
        return first, values - first

    for step in range(STEPS):
        for base, span in parts:
            if step or base is not bases[0]:
                fill_slots(step, base)
            for j in span:
                group_copy(step, j, False).start()
        if step:
            fill_edges(step)
        for copy in edge_copies(step):
            copy.start()

        if step == 0:
            loads[3].wait()
            words = sum(math.prod(dst.shape) for dst in (
                corner_in, grad_in, angles_in, mass_in, volume_in, nodes_in, facets_in, mask_in,
            ))
            drain(column_buf.at[pl.ds(0, words // LANES)], in_sem.at[4])
            for copy in prev_copies():
                copy.start()
            for i in range(rows):
                cols = pl.ds(i * LANES, LANES)
                stress[pl.ds(i, 3, stride=rows), :] = stress_in[:, cols]
                corner[pl.ds(i, 4, stride=rows), :] = corner_in[:, cols]
                grad[pl.ds(i, 8, stride=rows), :] = grad_in[:, cols]
                angle[pl.ds(i, 2, stride=rows), :] = angles_in[:, cols]
            tile_ids[...] = jnp.zeros_like(tile_ids)
            for t in range(tiles):
                tile_ids[pl.ds(5 * t, 1), :] = nodes_in[pl.ds(t, 1), :]
                for a in range(4):
                    tile_ids[pl.ds(5 * t + 1 + a, 1), :] = facets_in[a, pl.ds(t, 1), :]
                live = jnp.where(t < count_in[0], 1.0, 0.0)
                weight_in[t] = mask_in[t].astype(F32) * live
            first_row = lax.broadcasted_iota(jnp.int32, (rows, LANES), 0) * LANES
            corner_low, corner_far = [], []
            for a in range(4):
                local = corner[pl.ds(a * rows, rows), :] - first_row
                corner_low.append(local & (LANES - 1))
                corner_far.append(local >= LANES)
                for i in range(rows):
                    hot = (sub == corner_low[a][i : i + 1]).astype(F32).astype(BF16)
                    win_hot[i, :, pl.ds(a * LANES, LANES)] = hot
            polar, azim = angle[pl.ds(0, rows), :], angle[pl.ds(rows, rows), :]

            def frame(polar, azim):
                cos_p, sin_p, cos_a, sin_a = jnp.cos(polar), jnp.sin(polar), jnp.cos(azim), jnp.sin(azim)
                return (cos_p * cos_a, cos_p * sin_a, -sin_p), (-sin_a, cos_a)

            volume = volume_in[...]
            pace = TIME_STEP / mass_in[...]
            gx = [grad[pl.ds(a * rows, rows), :] for a in range(4)]
            gy = [grad[pl.ds((4 + a) * rows, rows), :] for a in range(4)]
            own = (frame(polar, azim), volume, gx, gy, corner_low, corner_far)
            slots_high = tile_ids[...] // cap
            slots_low = tile_ids[...] % cap
            low_columns = jnp.transpose(slots_low)
            node_columns = jnp.transpose(send_in[0] & (LANES - 1))
            for g in range(group):
                column_buf[pl.ds(g * cap, cap), :] = jnp.broadcast_to(node_columns[:, g : g + 1], (cap, LANES))
            for b in range(5 * tiles):
                cols = pl.ds(b * LANES, LANES)
                for half in range(halves):
                    span = pl.ds(half * LANES, LANES)
                    hot = sub + half * LANES == slots_low[b : b + 1]
                    look_hot[span, cols] = hot.astype(F32).astype(F8)
                    hot = lane + half * LANES == low_columns[:, b : b + 1]
                    slot_hot[cols, span] = hot.astype(F32).astype(F8)
            for n, g in enumerate(arrival):
                hot = lane_tall == column_buf[pl.ds(pl.multiple_of(g * cap, cap), cap), :]
                node_hot[pl.ds(n * cap, cap), :] = hot.astype(F32).astype(F8)

        mine, landed = (send_buf, recv_buf) if step == 0 else (again_buf.at[step - 1], fresh_buf.at[step - 1])
        landed[my_place] = mine[my_place]
        depth = 6 if step == 0 else 3
        deep = 16 if step == 0 else 8
        taken = [[jnp.zeros((8, LANES), F32)] * (deep // 8) for b in range(5 * tiles)]
        for far, base in ((0, bases[1]), (1, bases[0])):
            landing = far_count if far else count - far_count
            drain(landed.at[pl.ds(0, landing), pl.ds(0, depth)], out_sem.at[step, far])
            table = []
            for g in range(segment):
                first, second = split(landed[base + g])
                if step == 0:
                    table += [first, second]
                else:
                    table.append(jnp.where(eight_wide < 4, first, jnp.roll(second, 4, axis=0)))
            table = jnp.concatenate(table, axis=0).astype(BF16)
            for b in range(0, 5 * tiles, 2):
                looked = nn_dot(table, look_hot[:, pl.ds(b * LANES, 2 * LANES)])
                for side in range(2):
                    high = jnp.broadcast_to(slots_high[b + side : b + side + 1] - base, (8, LANES))
                    block = looked[:, side * LANES : (side + 1) * LANES]
                    for g in range(segment):
                        match = high == g
                        taken[b + side] = [
                            jnp.where(match, block[g * deep + 8 * p : g * deep + 8 * p + 8], old)
                            for p, old in enumerate(taken[b + side])
                        ]
        state = [t[0] + (t[1] if step == 0 else jnp.roll(t[0], 4, axis=0)) for t in taken]
        slots = jnp.zeros((6 * group, cap), F32)
        bodies = {}
        for t in range(tiles):
            bodies[t, 0] = state[5 * t]
            bodies[t, 1] = 0.25 * sum(state[5 * t + 1 + a] for a in range(4))
        if step:
            for at in bodies:
                moved = old_bodies[at] + TIME_STEP * jnp.roll(bodies[at], 3, axis=0)
                bodies[at] = jnp.where(eight < 3, bodies[at], moved)
        old_bodies = bodies
        tall, blocks_wide = [], []
        for t in range(tiles):
            high_part, rest = split(bodies[t, 0])
            mid_part, low_part = split(rest)
            tall.append(jnp.where(
                eight % 4 == 3, 1.0,
                jnp.where(eight < 3, jnp.roll(high_part, 5, axis=0), jnp.roll(mid_part, 1, axis=0)),
            ))
            tall.append(jnp.where(eight < 3, jnp.roll(low_part, 5, axis=0), jnp.where(eight == 3, 1.0, 0.0)))
            high_part, rest = split(-bodies[t, 1])
            mid_part, low_part = split(rest)
            for k in range(3):
                unit = jnp.where(eight % 4 == k, 1.0, 0.0)
                spread = [jnp.broadcast_to(p[3 + k : 4 + k], (8, LANES)) for p in (high_part, mid_part, low_part)]
                block = [
                    jnp.where(eight == 3, spread[0], jnp.where(eight == 7, spread[1], unit)),
                    jnp.where(eight == 3, spread[2], jnp.where(eight < 3, unit, 0.0)),
                ]
                none = [jnp.zeros((16, LANES), F32)]
                blocks_wide.append(jnp.concatenate(none * t + block + none * (tiles - 1 - t), axis=0))
        gaps = nn_dot(
            jnp.transpose(jnp.concatenate(tall, axis=0)).astype(BF16),
            jnp.concatenate(blocks_wide, axis=1).astype(BF16),
        )
        dots = []
        for t in range(tiles):
            mixes = [
                jnp.where(
                    eight < 3, STIFFNESS * jnp.roll(bodies[t, s], 5, axis=0) - DAMPING * bodies[t, s], 0.0
                )
                for s in range(2)
            ]
            left_a, left_b = [
                jnp.concatenate(two_parts(jnp.where(eight == 3, 1.0, mix)), axis=0) for mix in mixes
            ]
            dist = jnp.zeros((LANES, LANES), F32)
            for k in range(3):
                at = (3 * t + k) * LANES
                gap = gaps[:, at : at + LANES]
                dist += gap * gap
            w1, w2 = two_parts(weight_in[t] * jnp.maximum(RADIUS_SQ - dist, 0.0))
            to_facet = nn_dot(
                jnp.concatenate([left_a, left_a], axis=1), jnp.concatenate([w1, w2], axis=0)
            )
            to_node = nt_dot(
                jnp.concatenate([left_b, left_b], axis=1), jnp.concatenate([w1, w2], axis=1)
            )
            dots.append((mixes, to_facet, to_node))
        for t in range(tiles):
            mixes, to_facet, to_node = dots[t]
            to_facet = to_facet[:8] + to_facet[8:]
            to_node = to_node[:8] + to_node[8:]
            node_force = mixes[0] * to_node[3:4] - to_node
            facet_force = -0.25 * (to_facet - to_facet[3:4] * mixes[1])
            for force, blocks in ((node_force, [5 * t]), (facet_force, [5 * t + 1 + a for a in range(4)])):
                matches = [group_iota == slots_high[b : b + 1] for b in blocks]
                for part, value in enumerate(split(force)):
                    for k in range(3):
                        row = jnp.broadcast_to(value[k : k + 1], (group, LANES))
                        for b, match in zip(blocks, matches):
                            tile_lhs[pl.ds((part * 3 + k) * group, group), pl.ds(b * LANES, LANES)] = (
                                jnp.where(match, row, 0.0).astype(BF16)
                            )
        slots = nn_dot(tile_lhs[...], slot_hot[...])
        slots = slots[: 3 * group] + slots[3 * group :]
        for k in range(3):
            back_buf[step, :, k, :] = slots[k * group : (k + 1) * group]
        for j in range(count):
            group_copy(step, j, True).start()

        if step == 0:
            drain(force_rows.at[pl.ds(0, 18)], edge_sem.at[STEPS])

            def whole(row):
                return jnp.broadcast_to(row, (8, LANES))

            prev_low, prev_far = [], []
            for a in range(4):
                local = corner_prev[pl.ds(a, 1), :] - (rows - 1) * LANES
                low = local & (LANES - 1)
                win_hot[rows, :, pl.ds(a * LANES, LANES)] = (sub == low).astype(F32).astype(BF16)
                prev_low.append(whole(low))
                prev_far.append(whole(local) >= LANES)
            prev = (
                frame(whole(angles_prev[pl.ds(0, 1), :]), whole(angles_prev[pl.ds(1, 1), :])),
                whole(volume_prev[...]),
                [whole(grad_prev[pl.ds(a, 1), :]) for a in range(4)],
                [whole(grad_prev[pl.ds(4 + a, 1), :]) for a in range(4)],
                prev_low, prev_far,
            )
            own_stress = [stress[pl.ds(k * rows, rows), :] for k in range(3)]
            prev_stress = [whole(stress_prev[pl.ds(k, 1), :]) for k in range(3)]

        def element_forces(batch, tension, near, far):
            (one, two), volume, gx, gy, low, beyond = batch
            corner_vel = [
                [
                    jnp.where(beyond[a], lane_take(far[k], low[a]), lane_take(near[k], low[a]))
                    for a in range(4)
                ]
                for k in range(3)
            ]
            xx = yy = xy = jnp.zeros(volume.shape, F32)
            for a in range(4):
                u = sum(one[k] * corner_vel[k][a] for k in range(3))
                w = sum(two[k] * corner_vel[k][a] for k in range(2))
                xx += gx[a] * u
                yy += gy[a] * w
                xy += gy[a] * u + gx[a] * w
            factor = TIME_STEP * YOUNG_MOD / (1.0 - POISSON * POISSON)
            sxx = tension[0] + factor * (xx + POISSON * yy)
            syy = tension[1] + factor * (POISSON * xx + yy)
            sxy = tension[2] + factor * 0.5 * (1.0 - POISSON) * xy
            hour = [
                HOURGLASS * volume
                * (corner_vel[k][0] - corner_vel[k][1] + corner_vel[k][2] - corner_vel[k][3])
                for k in range(3)
            ]
            forces = []
            for a in range(4):
                f1 = -volume * (gx[a] * sxx + gy[a] * sxy)
                f2 = -volume * (gy[a] * syy + gx[a] * sxy)
                parts = []
                for k in range(3):
                    force = one[k] * f1 - (1.0 if a % 2 == 0 else -1.0) * hour[k]
                    if k < 2:
                        force += two[k] * f2
                    first = force.astype(BF16).astype(F32)
                    parts.append((first, force - first))
                forces.append(parts)
            return [sxx, syy, sxy], forces

        drain(edge_recv.at[step], edge_sem.at[step])
        for k in range(3):
            vel[pl.ds(k * 2 * rows + rows, 1), :] = edge_recv[step, 0, pl.ds(k, 1), :]
        own_stress, forces = element_forces(
            own, own_stress,
            [velocity_rows(k) for k in range(3)],
            [vel[pl.ds(k * 2 * rows + 1, rows), :] for k in range(3)],
        )
        prev_stress, prev_forces = element_forces(
            prev, prev_stress,
            [whole(edge_recv[step, 1, pl.ds(k, 1), :]) for k in range(3)],
            [whole(vel[pl.ds(k * 2 * rows, 1), :]) for k in range(3)],
        )
        for a in range(4):
            for k in range(3):
                for part in range(2):
                    for side in range(2):
                        at = part * 8 + k * 2 + side
                        keep = corner_far[a] if side else jnp.logical_not(corner_far[a])
                        win_rows[a, pl.ds(at, rows, stride=16), :] = jnp.where(
                            keep, forces[a][k][part], 0.0
                        )
                        far_row = jnp.where(prev_far[a], prev_forces[a][k][part], 0.0)[:1]
                        win_rows[a, pl.ds(rows * 16 + at, 1), :] = far_row
        for i in range(rows + 1):
            left = jnp.concatenate(
                [win_rows[a, pl.ds(i * 16, 16), :].astype(BF16) for a in range(4)], axis=1
            )
            summed = nt_dot(left, win_hot[i])
            force_rows[pl.ds(i * 8, 8), :] = summed[:8] + summed[8:]
        internal = []
        for k in range(3):
            near = force_rows[pl.ds(k * 2, rows, stride=8), :]
            far = force_rows[pl.ds(k * 2 + 1, rows - 1, stride=8), :]
            edge_row = force_rows[pl.ds(rows * 8 + k * 2 + 1, 1), :]
            internal.append(near + jnp.concatenate([edge_row, far], axis=0))
        if step + 1 == STEPS:
            for k in range(3):
                for i in range(rows):
                    stress_out[pl.ds(k, 1), pl.ds(i * LANES, LANES)] = own_stress[k][i : i + 1]
        if step + 1 == STEPS:
            sent = count * halves * (6 + 3 * (STEPS - 1) + 3 * STEPS) + 6 * STEPS + 18
            drain(column_buf.at[pl.ds(0, sent)], send_sem.at[0])
        contact = jnp.zeros((3 * rows, LANES), F32)
        for begin in range(0, group, batch):
            answers = batch - 1 if begin == 0 else batch
            drain(answer_buf.at[step, pl.ds(0, answers), pl.ds(0, 3)], back_sem.at[step, int(begin > 0)])
            for n in range(begin, begin + batch):
                g = arrival[n]
                source = answer_buf if n else back_buf
                halved = split(source[step, g])
                for half in range(halves):
                    match = row_iota == slot_ids[g, pl.ds(half, 1), :]
                    at = pl.ds((n * halves + half) * LANES, LANES)
                    for part in range(2):
                        for k in range(3):
                            row = halved[part][k : k + 1, half * LANES : (half + 1) * LANES]
                            chosen = jnp.where(match, jnp.broadcast_to(row, match.shape), 0.0)
                            pairs[pl.ds((part * 3 + k) * rows, rows), at] = chosen.astype(BF16)
            at = pl.ds(begin * cap, batch * cap)
            summed = nn_dot(pairs[:, at], node_hot[at, :])
            contact += summed[: 3 * rows] + summed[3 * rows :]
        for k in range(3):
            fresh = velocity_rows(k) + pace * (internal[k] + contact[k * rows : (k + 1) * rows])
            vel[pl.ds(k * 2 * rows, rows), :] = fresh
            pos[pl.ds(k * rows, rows), :] = pos[pl.ds(k * rows, rows), :] + TIME_STEP * fresh

    for i in range(rows):
        cols = pl.ds(i * LANES, LANES)
        coords_out[:, cols] = pos[pl.ds(i, 3, stride=rows), :]
        velocity_out[:, cols] = vel[pl.ds(i, 3, stride=2 * rows), :]


def put_out(coords_in, velocity_in, stress_in, coords_out, velocity_out, stress_out, sems):
    pairs = ((coords_in, coords_out), (velocity_in, velocity_out), (stress_in, stress_out))
    copies = [pltpu.make_async_copy(src, dst, sems.at[n]) for n, (src, dst) in enumerate(pairs)]
    for copy in copies:
        copy.start()
    for copy in copies:
        copy.wait()


def per_device(
    sizes, coords, velocity, node_mass, corner_nodes, shape_grad, frame_angles, volume, stress,
    send_nodes, tile_count, tile_nodes, tile_facets, pair_mask,
):
    count = coords.shape[1]
    rows = count // LANES
    group = sizes[1] * sizes[2]
    cap = send_nodes.shape[2]
    tiles = tile_nodes.shape[0]
    vmem = pl.BlockSpec(memory_space=pltpu.VMEM)
    hbm = pl.BlockSpec(memory_space=pltpu.HBM)
    state = jax.ShapeDtypeStruct((3, count), F32)
    halves = cap // LANES
    arrays = (
        coords, velocity, node_mass.reshape(rows, LANES), corner_nodes, shape_grad, frame_angles,
        volume.reshape(rows, LANES), stress, send_nodes, tile_nodes, tile_facets, pair_mask,
    )
    arrays = tuple(pltpu.with_memory_space_constraint(a, pltpu.HBM) for a in arrays)
    dma = pltpu.SemaphoreType.DMA
    finals = pl.pallas_call(
        functools.partial(kernel, sizes),
        out_shape=(state, state, state),
        in_specs=[hbm] * 12 + [pl.BlockSpec(memory_space=pltpu.SMEM)],
        out_specs=(vmem, vmem, vmem),
        scratch_shapes=[pltpu.VMEM(a.shape, a.dtype) for a in arrays] + [
            dma((5,)),
            pltpu.VMEM((3 * rows, LANES), F32),
            pltpu.VMEM((6 * rows, LANES), F32),
            pltpu.VMEM((4 * rows, LANES), jnp.int32),
            pltpu.VMEM((8 * rows, LANES), F32),
            pltpu.VMEM((3 * rows, LANES), F32),
            pltpu.VMEM((2 * rows, LANES), F32),
            pltpu.VMEM((group, halves, LANES), jnp.int32),
            pltpu.VMEM((-(-5 * tiles // 8) * 8, LANES), jnp.int32),
            pltpu.VMEM((rows + 1, LANES, 4 * LANES), BF16),
            pltpu.VMEM((cap, 5 * tiles * LANES), F8),
            pltpu.VMEM((5 * tiles * LANES, cap), F8),
            pltpu.VMEM((group * cap, LANES), F8),
            pltpu.VMEM((4, 16 * (rows + 1), LANES), F32),
            pltpu.VMEM((8 * (rows + 1), LANES), F32),
            pltpu.VMEM((6 * group, 5 * tiles * LANES), BF16),
            pltpu.VMEM((6 * rows, group * cap), BF16),
            pltpu.VMEM((group * cap, LANES), jnp.int32),
            pltpu.VMEM((tiles, LANES, LANES), F32),
            pltpu.VMEM((group, 8, cap), F32),
            pltpu.VMEM((group, 8, cap), F32),
            pltpu.VMEM((STEPS - 1, group, 8, cap), F32),
            pltpu.VMEM((STEPS - 1, group, 8, cap), F32),
            pltpu.VMEM((STEPS, group, 4, cap), F32),
            pltpu.VMEM((STEPS, group, 4, cap), F32),
            pltpu.VMEM((STEPS - 1, 3, LANES), F32),
            pltpu.VMEM((STEPS - 1, 3, LANES), F32),
            pltpu.VMEM((STEPS, 2, 3, LANES), F32),
            pltpu.VMEM((4, LANES), jnp.int32),
            pltpu.VMEM((8, LANES), F32),
            pltpu.VMEM((2, LANES), F32),
            pltpu.VMEM((1, LANES), F32),
            pltpu.VMEM((3, LANES), F32),
            dma((1,)),
            dma((STEPS, 2)),
            dma((STEPS, 2)),
            dma((STEPS + 1,)),
        ],
        compiler_params=pltpu.CompilerParams(
            collective_id=0, has_side_effects=True, vmem_limit_bytes=24 * 1024 * 1024
        ),
    )(*arrays, tile_count)
    return pl.pallas_call(
        put_out,
        out_shape=(state, state, state),
        in_specs=[vmem] * 3,
        out_specs=(hbm, hbm, hbm),
        scratch_shapes=[dma((3,))],
        compiler_params=pltpu.CompilerParams(vmem_limit_bytes=1024 * 1024),
    )(*finals)


def solution(mesh):
    axes = ("len", "wid", "dep")
    flat, wide = P(axes), P(None, axes)
    sizes = tuple(mesh.shape[name] for name in axes)
    return jax.shard_map(
        functools.partial(per_device, sizes),
        mesh=mesh,
        in_specs=(
            wide, wide, flat, wide, wide, wide, flat, wide,
            P(axes, None, None), flat, P(axes, None), P(None, axes, None), P(axes, None, None),
        ),
        out_specs=(wide, wide, wide),
        check_vma=False,
    )
```

```python
import functools
import math

import jax
import jax.numpy as jnp
from jax import lax
from jax.experimental import pallas as pl
from jax.experimental.pallas import tpu as pltpu
from jax.sharding import PartitionSpec as P

STEPS = 2
TIME_STEP = 0.1
YOUNG_MOD = 1.0
POISSON = 0.3
HOURGLASS = 0.1
RADIUS_SQ = 1.0
STIFFNESS = 0.1
DAMPING = 0.05

LANES = 128
MESH = pl.DeviceIdType.MESH
F32 = jnp.float32
BF16 = jnp.bfloat16
F8 = jnp.float8_e4m3fn


def two_parts(values):
    first = values.astype(BF16)
    return first, (values - first.astype(F32)).astype(BF16)


def lane_take(table, low):
    return jnp.take_along_axis(table, low, axis=1, mode="promise_in_bounds")


def nt_dot(left, right):
    return lax.dot_general(left, right, (((1,), (1,)), ((), ())), preferred_element_type=F32)


def nn_dot(left, right):
    return lax.dot_general(left, right, (((1,), (0,)), ((), ())), preferred_element_type=F32)


def kernel(
    sizes,
    coords_hbm, velocity_hbm, mass_hbm, corner_hbm, grad_hbm, angles_hbm, volume_hbm, stress_hbm,
    send_hbm, nodes_hbm, facets_hbm, mask_hbm, count_in,
    coords_out, velocity_out, stress_out,
    coords_in, velocity_in, mass_in, corner_in, grad_in, angles_in, volume_in, stress_in,
    send_in, nodes_in, facets_in, mask_in, in_sem,
    pos, vel, corner, grad, stress, angle, slot_ids, tile_ids, win_hot, look_hot, slot_hot, node_hot,
    win_rows, force_rows, tile_lhs, pairs, column_buf, weight_in,
    send_buf, recv_buf, again_buf, fresh_buf, back_buf, answer_buf,
    first_buf, last_buf, edge_recv,
    corner_prev, grad_prev, angles_prev, volume_prev, stress_prev,
    send_sem, out_sem, back_sem, edge_sem,
):
    n_len, n_wid, n_dep = sizes
    group = n_wid * n_dep
    devices = n_len * group
    rows = coords_in.shape[1] // LANES
    cap = send_in.shape[2]
    halves = cap // LANES
    tiles = nodes_in.shape[0]
    my_len = lax.axis_index("len")
    my_wid = lax.axis_index("wid")
    my_dep = lax.axis_index("dep")
    my_place = my_wid * n_dep + my_dep
    my_id = my_len * group + my_place

    def by_id(p):
        return (p // group, (p % group) // n_dep, p % n_dep)

    upper = (2 * my_wid) // n_wid
    shifts = sorted(range(1, n_dep), key=lambda d: -min(d, n_dep - d))
    peers = []
    for r in range(n_wid):
        across = r + (1 - upper) * (n_wid - 1 - 2 * r)
        for shift in shifts:
            peers.append((across, lax.rem(my_dep + shift, n_dep)))
        if r < n_wid - 1:
            up = r + (r - my_wid + n_wid) // n_wid
            down = n_wid - 1 - r - (my_wid - (n_wid - 1 - r) + n_wid) // n_wid
            peers.append((upper * up + (1 - upper) * down, my_dep))
    places = [wid * n_dep + dep for wid, dep in peers]
    count = group - 1
    arrival = [my_place] + places[::-1]

    before = by_id(lax.rem(my_id + devices - 1, devices))
    after = by_id(lax.rem(my_id + 1, devices))

    loads = [
        pltpu.make_async_copy(src, dst, in_sem.at[min(n, 4)])
        for n, (src, dst) in enumerate((
            (send_hbm, send_in), (velocity_hbm, velocity_in), (coords_hbm, coords_in),
            (stress_hbm, stress_in), (corner_hbm, corner_in), (grad_hbm, grad_in),
            (angles_hbm, angles_in), (mass_hbm, mass_in), (volume_hbm, volume_in),
            (nodes_hbm, nodes_in), (facets_hbm, facets_in), (mask_hbm, mask_in),
        ))
    ]
    for load in loads[:3]:
        load.start()
    barrier = pltpu.get_barrier_semaphore()
    for wid, dep in peers:
        pl.semaphore_signal(barrier, inc=1, device_id=(my_len, wid, dep), device_id_type=MESH)
    pl.semaphore_signal(barrier, inc=1, device_id=before, device_id_type=MESH)
    pl.semaphore_signal(barrier, inc=1, device_id=after, device_id_type=MESH)
    for load in loads[3:]:
        load.start()
    for load in loads[:3]:
        load.wait()
    for i in range(rows):
        cols = pl.ds(i * LANES, LANES)
        pos[pl.ds(i, 3, stride=rows), :] = coords_in[:, cols]
        for k in range(3):
            vel[pl.ds(k * 2 * rows + i, 1), :] = velocity_in[pl.ds(k, 1), cols]

    def velocity_rows(k):
        return vel[pl.ds(k * 2 * rows, rows), :]

    def fill_edges(step):
        for k in range(3):
            first_buf[step - 1, pl.ds(k, 1), :] = vel[pl.ds(k * 2 * rows, 1), :]
            last_buf[step - 1, pl.ds(k, 1), :] = vel[pl.ds(k * 2 * rows + rows - 1, 1), :]

    segment = group // 2
    bases = [pl.multiple_of(side * segment, segment) for side in (1 - upper, upper)]

    def fill_slots(step, base):
        tables = [velocity_rows(k) for k in range(3)]
        if step == 0:
            tables += [pos[pl.ds(k * rows, rows), :] for k in range(3)]
        target = send_buf if step == 0 else again_buf.at[step - 1]
        for half in range(halves):
            cols = pl.ds(half * LANES, LANES)
            ids = send_in[0, pl.ds(base, segment), cols]
            low, high = ids & (LANES - 1), ids >> 7
            if step == 0:
                slot_ids[pl.ds(base, segment), half, :] = high
            for c, table in enumerate(tables):
                found = jnp.zeros(ids.shape, F32)
                for h in range(rows):
                    row = jnp.broadcast_to(table[h : h + 1], ids.shape)
                    found = jnp.where(high == h, lane_take(row, low), found)
                target[pl.ds(base, segment), c, cols] = found

    def remote(src, dst, recv_sem, target):
        return pltpu.make_async_remote_copy(
            src_ref=src, dst_ref=dst, send_sem=send_sem.at[0], recv_sem=recv_sem,
            device_id=target, device_id_type=MESH,
        )

    def drain(ref, sem):
        pltpu.make_async_copy(ref, ref, sem).wait()

    final = pl.ds((rows - 1) * LANES, LANES)

    def edge_copies(step):
        if step == 0:
            first, last = velocity_in.at[:, pl.ds(0, LANES)], velocity_in.at[:, final]
        else:
            first, last = first_buf.at[step - 1], last_buf.at[step - 1]
        return (
            remote(first, edge_recv.at[step, 0], edge_sem.at[step], before),
            remote(last, edge_recv.at[step, 1], edge_sem.at[step], after),
        )

    def prev_copies():
        pairs = (
            (corner_in.at[:, final], corner_prev), (grad_in.at[:, final], grad_prev),
            (angles_in.at[:, final], angles_prev), (stress_in.at[:, final], stress_prev),
            (volume_in.at[pl.ds(rows - 1, 1), :], volume_prev),
        )
        return [
            remote(src, dst, edge_sem.at[STEPS], after) for src, dst in pairs
        ]

    far_count = n_dep * (n_wid // 2)

    def group_copy(step, j, back):
        wid, dep = peers[j]
        if back:
            src, dst, depth, sem = back_buf.at[step], answer_buf.at[step], 3, back_sem.at[0, int(j < far_count)]
        elif step == 0:
            src, dst, depth, sem = send_buf, recv_buf, 6, out_sem.at[0, int(j < far_count)]
        else:
            src, dst, depth, sem = again_buf.at[step - 1], fresh_buf.at[step - 1], 3, out_sem.at[0, int(j < far_count)]
        return remote(
            src.at[places[j], pl.ds(0, depth)], dst.at[my_place, pl.ds(0, depth)], sem, (my_len, wid, dep)
        )

    batch = count + 1 - far_count
    parts = ((bases[0], range(far_count)), (bases[1], range(far_count, count)))

    fill_slots(0, bases[0])
    pl.semaphore_wait(barrier, group + 1)

    sub = lax.broadcasted_iota(jnp.int32, (LANES, LANES), 0)
    lane = lax.broadcasted_iota(jnp.int32, (LANES, LANES), 1)
    lane_tall = lax.broadcasted_iota(jnp.int32, (cap, LANES), 1)
    eight = lax.broadcasted_iota(jnp.int32, (8, LANES), 0)
    row_iota = lax.broadcasted_iota(jnp.int32, (rows, LANES), 0)
    eight_wide = lax.broadcasted_iota(jnp.int32, (8, cap), 0)
    group_iota = lax.broadcasted_iota(jnp.int32, (group, LANES), 0)

    def split(values):
        first = values.astype(BF16).astype(F32)
        return first, values - first

    for step in range(STEPS):
        for base, span in parts:
            if step or base is not bases[0]:
                fill_slots(step, base)
            for j in span:
                group_copy(step, j, False).start()
        if step:
            fill_edges(step)
        for copy in edge_copies(step):
            copy.start()

        if step == 0:
            loads[3].wait()
            words = sum(math.prod(dst.shape) for dst in (
                corner_in, grad_in, angles_in, mass_in, volume_in, nodes_in, facets_in, mask_in,
            ))
            drain(column_buf.at[pl.ds(0, words // LANES)], in_sem.at[4])
            for copy in prev_copies():
                copy.start()
            for i in range(rows):
                cols = pl.ds(i * LANES, LANES)
                stress[pl.ds(i, 3, stride=rows), :] = stress_in[:, cols]
                corner[pl.ds(i, 4, stride=rows), :] = corner_in[:, cols]
                grad[pl.ds(i, 8, stride=rows), :] = grad_in[:, cols]
                angle[pl.ds(i, 2, stride=rows), :] = angles_in[:, cols]
            tile_ids[...] = jnp.zeros_like(tile_ids)
            for t in range(tiles):
                tile_ids[pl.ds(5 * t, 1), :] = nodes_in[pl.ds(t, 1), :]
                for a in range(4):
                    tile_ids[pl.ds(5 * t + 1 + a, 1), :] = facets_in[a, pl.ds(t, 1), :]
                live = jnp.where(t < count_in[0], 1.0, 0.0)
                weight_in[t] = mask_in[t].astype(F32) * live
            first_row = lax.broadcasted_iota(jnp.int32, (rows, LANES), 0) * LANES
            corner_low, corner_far = [], []
            for a in range(4):
                local = corner[pl.ds(a * rows, rows), :] - first_row
                corner_low.append(local & (LANES - 1))
                corner_far.append(local >= LANES)
                for i in range(rows):
                    hot = (sub == corner_low[a][i : i + 1]).astype(F32).astype(BF16)
                    win_hot[i, :, pl.ds(a * LANES, LANES)] = hot
            polar, azim = angle[pl.ds(0, rows), :], angle[pl.ds(rows, rows), :]

            def frame(polar, azim):
                cos_p, sin_p, cos_a, sin_a = jnp.cos(polar), jnp.sin(polar), jnp.cos(azim), jnp.sin(azim)
                return (cos_p * cos_a, cos_p * sin_a, -sin_p), (-sin_a, cos_a)

            volume = volume_in[...]
            pace = TIME_STEP / mass_in[...]
            gx = [grad[pl.ds(a * rows, rows), :] for a in range(4)]
            gy = [grad[pl.ds((4 + a) * rows, rows), :] for a in range(4)]
            own = (frame(polar, azim), volume, gx, gy, corner_low, corner_far)
            slots_high = tile_ids[...] // cap
            slots_low = tile_ids[...] % cap
            low_columns = jnp.transpose(slots_low)
            node_columns = jnp.transpose(send_in[0] & (LANES - 1))
            for g in range(group):
                column_buf[pl.ds(g * cap, cap), :] = jnp.broadcast_to(node_columns[:, g : g + 1], (cap, LANES))
            for b in range(5 * tiles):
                cols = pl.ds(b * LANES, LANES)
                for half in range(halves):
                    span = pl.ds(half * LANES, LANES)
                    hot = sub + half * LANES == slots_low[b : b + 1]
                    look_hot[span, cols] = hot.astype(F32).astype(F8)
                    hot = lane + half * LANES == low_columns[:, b : b + 1]
                    slot_hot[cols, span] = hot.astype(F32).astype(F8)
            for n, g in enumerate(arrival):
                hot = lane_tall == column_buf[pl.ds(pl.multiple_of(g * cap, cap), cap), :]
                node_hot[pl.ds(n * cap, cap), :] = hot.astype(F32).astype(F8)

        mine, landed = (send_buf, recv_buf) if step == 0 else (again_buf.at[step - 1], fresh_buf.at[step - 1])
        landed[my_place] = mine[my_place]
        depth = 6 if step == 0 else 3
        deep = 16 if step == 0 else 8
        taken = [[jnp.zeros((8, LANES), F32)] * (deep // 8) for b in range(5 * tiles)]
        for far, base in ((0, bases[1]), (1, bases[0])):
            landing = far_count if far else count - far_count
            drain(landed.at[pl.ds(0, landing), pl.ds(0, depth)], out_sem.at[0, far])
            table = []
            for g in range(segment):
                first, second = split(landed[base + g])
                if step == 0:
                    table += [first, second]
                else:
                    table.append(jnp.where(eight_wide < 4, first, jnp.roll(second, 4, axis=0)))
            table = jnp.concatenate(table, axis=0).astype(BF16)
            for b in range(0, 5 * tiles, 2):
                looked = nn_dot(table, look_hot[:, pl.ds(b * LANES, 2 * LANES)])
                for side in range(2):
                    high = jnp.broadcast_to(slots_high[b + side : b + side + 1] - base, (8, LANES))
                    block = looked[:, side * LANES : (side + 1) * LANES]
                    for g in range(segment):
                        match = high == g
                        taken[b + side] = [
                            jnp.where(match, block[g * deep + 8 * p : g * deep + 8 * p + 8], old)
                            for p, old in enumerate(taken[b + side])
                        ]
        state = [t[0] + (t[1] if step == 0 else jnp.roll(t[0], 4, axis=0)) for t in taken]
        slots = jnp.zeros((6 * group, cap), F32)
        bodies = {}
        for t in range(tiles):
            bodies[t, 0] = state[5 * t]
            bodies[t, 1] = 0.25 * sum(state[5 * t + 1 + a] for a in range(4))
        if step:
            for at in bodies:
                moved = old_bodies[at] + TIME_STEP * jnp.roll(bodies[at], 3, axis=0)
                bodies[at] = jnp.where(eight < 3, bodies[at], moved)
        old_bodies = bodies
        tall, blocks_wide = [], []
        for t in range(tiles):
            high_part, rest = split(bodies[t, 0])
            mid_part, low_part = split(rest)
            tall.append(jnp.where(
                eight % 4 == 3, 1.0,
                jnp.where(eight < 3, jnp.roll(high_part, 5, axis=0), jnp.roll(mid_part, 1, axis=0)),
            ))
            tall.append(jnp.where(eight < 3, jnp.roll(low_part, 5, axis=0), jnp.where(eight == 3, 1.0, 0.0)))
            high_part, rest = split(-bodies[t, 1])
            mid_part, low_part = split(rest)
            for k in range(3):
                unit = jnp.where(eight % 4 == k, 1.0, 0.0)
                spread = [jnp.broadcast_to(p[3 + k : 4 + k], (8, LANES)) for p in (high_part, mid_part, low_part)]
                block = [
                    jnp.where(eight == 3, spread[0], jnp.where(eight == 7, spread[1], unit)),
                    jnp.where(eight == 3, spread[2], jnp.where(eight < 3, unit, 0.0)),
                ]
                none = [jnp.zeros((16, LANES), F32)]
                blocks_wide.append(jnp.concatenate(none * t + block + none * (tiles - 1 - t), axis=0))
        gaps = nn_dot(
            jnp.transpose(jnp.concatenate(tall, axis=0)).astype(BF16),
            jnp.concatenate(blocks_wide, axis=1).astype(BF16),
        )
        dots = []
        for t in range(tiles):
            mixes = [
                jnp.where(
                    eight < 3, STIFFNESS * jnp.roll(bodies[t, s], 5, axis=0) - DAMPING * bodies[t, s], 0.0
                )
                for s in range(2)
            ]
            left_a, left_b = [
                jnp.concatenate(two_parts(jnp.where(eight == 3, 1.0, mix)), axis=0) for mix in mixes
            ]
            dist = jnp.zeros((LANES, LANES), F32)
            for k in range(3):
                at = (3 * t + k) * LANES
                gap = gaps[:, at : at + LANES]
                dist += gap * gap
            w1, w2 = two_parts(weight_in[t] * jnp.maximum(RADIUS_SQ - dist, 0.0))
            to_facet = nn_dot(
                jnp.concatenate([left_a, left_a], axis=1), jnp.concatenate([w1, w2], axis=0)
            )
            to_node = nt_dot(
                jnp.concatenate([left_b, left_b], axis=1), jnp.concatenate([w1, w2], axis=1)
            )
            dots.append((mixes, to_facet, to_node))
        for t in range(tiles):
            mixes, to_facet, to_node = dots[t]
            to_facet = to_facet[:8] + to_facet[8:]
            to_node = to_node[:8] + to_node[8:]
            node_force = mixes[0] * to_node[3:4] - to_node
            facet_force = -0.25 * (to_facet - to_facet[3:4] * mixes[1])
            for force, blocks in ((node_force, [5 * t]), (facet_force, [5 * t + 1 + a for a in range(4)])):
                matches = [group_iota == slots_high[b : b + 1] for b in blocks]
                for part, value in enumerate(split(force)):
                    for k in range(3):
                        row = jnp.broadcast_to(value[k : k + 1], (group, LANES))
                        for b, match in zip(blocks, matches):
                            tile_lhs[pl.ds((part * 3 + k) * group, group), pl.ds(b * LANES, LANES)] = (
                                jnp.where(match, row, 0.0).astype(BF16)
                            )
        slots = nn_dot(tile_lhs[...], slot_hot[...])
        slots = slots[: 3 * group] + slots[3 * group :]
        for k in range(3):
            back_buf[step, :, k, :] = slots[k * group : (k + 1) * group]
        for j in range(count):
            group_copy(step, j, True).start()

        if step == 0:
            drain(force_rows.at[pl.ds(0, 18)], edge_sem.at[STEPS])

            def whole(row):
                return jnp.broadcast_to(row, (8, LANES))

            prev_low, prev_far = [], []
            for a in range(4):
                local = corner_prev[pl.ds(a, 1), :] - (rows - 1) * LANES
                low = local & (LANES - 1)
                win_hot[rows, :, pl.ds(a * LANES, LANES)] = (sub == low).astype(F32).astype(BF16)
                prev_low.append(whole(low))
                prev_far.append(whole(local) >= LANES)
            prev = (
                frame(whole(angles_prev[pl.ds(0, 1), :]), whole(angles_prev[pl.ds(1, 1), :])),
                whole(volume_prev[...]),
                [whole(grad_prev[pl.ds(a, 1), :]) for a in range(4)],
                [whole(grad_prev[pl.ds(4 + a, 1), :]) for a in range(4)],
                prev_low, prev_far,
            )
            own_stress = [stress[pl.ds(k * rows, rows), :] for k in range(3)]
            prev_stress = [whole(stress_prev[pl.ds(k, 1), :]) for k in range(3)]

        def element_forces(batch, tension, near, far):
            (one, two), volume, gx, gy, low, beyond = batch
            corner_vel = [
                [
                    jnp.where(beyond[a], lane_take(far[k], low[a]), lane_take(near[k], low[a]))
                    for a in range(4)
                ]
                for k in range(3)
            ]
            xx = yy = xy = jnp.zeros(volume.shape, F32)
            for a in range(4):
                u = sum(one[k] * corner_vel[k][a] for k in range(3))
                w = sum(two[k] * corner_vel[k][a] for k in range(2))
                xx += gx[a] * u
                yy += gy[a] * w
                xy += gy[a] * u + gx[a] * w
            factor = TIME_STEP * YOUNG_MOD / (1.0 - POISSON * POISSON)
            sxx = tension[0] + factor * (xx + POISSON * yy)
            syy = tension[1] + factor * (POISSON * xx + yy)
            sxy = tension[2] + factor * 0.5 * (1.0 - POISSON) * xy
            hour = [
                HOURGLASS * volume
                * (corner_vel[k][0] - corner_vel[k][1] + corner_vel[k][2] - corner_vel[k][3])
                for k in range(3)
            ]
            forces = []
            for a in range(4):
                f1 = -volume * (gx[a] * sxx + gy[a] * sxy)
                f2 = -volume * (gy[a] * syy + gx[a] * sxy)
                parts = []
                for k in range(3):
                    force = one[k] * f1 - (1.0 if a % 2 == 0 else -1.0) * hour[k]
                    if k < 2:
                        force += two[k] * f2
                    first = force.astype(BF16).astype(F32)
                    parts.append((first, force - first))
                forces.append(parts)
            return [sxx, syy, sxy], forces

        drain(edge_recv.at[step], edge_sem.at[step])
        for k in range(3):
            vel[pl.ds(k * 2 * rows + rows, 1), :] = edge_recv[step, 0, pl.ds(k, 1), :]
        own_stress, forces = element_forces(
            own, own_stress,
            [velocity_rows(k) for k in range(3)],
            [vel[pl.ds(k * 2 * rows + 1, rows), :] for k in range(3)],
        )
        prev_stress, prev_forces = element_forces(
            prev, prev_stress,
            [whole(edge_recv[step, 1, pl.ds(k, 1), :]) for k in range(3)],
            [whole(vel[pl.ds(k * 2 * rows, 1), :]) for k in range(3)],
        )
        for a in range(4):
            for k in range(3):
                for part in range(2):
                    for side in range(2):
                        at = part * 8 + k * 2 + side
                        keep = corner_far[a] if side else jnp.logical_not(corner_far[a])
                        win_rows[a, pl.ds(at, rows, stride=16), :] = jnp.where(
                            keep, forces[a][k][part], 0.0
                        )
                        far_row = jnp.where(prev_far[a], prev_forces[a][k][part], 0.0)[:1]
                        win_rows[a, pl.ds(rows * 16 + at, 1), :] = far_row
        for i in range(rows + 1):
            left = jnp.concatenate(
                [win_rows[a, pl.ds(i * 16, 16), :].astype(BF16) for a in range(4)], axis=1
            )
            summed = nt_dot(left, win_hot[i])
            force_rows[pl.ds(i * 8, 8), :] = summed[:8] + summed[8:]
        internal = []
        for k in range(3):
            near = force_rows[pl.ds(k * 2, rows, stride=8), :]
            far = force_rows[pl.ds(k * 2 + 1, rows - 1, stride=8), :]
            edge_row = force_rows[pl.ds(rows * 8 + k * 2 + 1, 1), :]
            internal.append(near + jnp.concatenate([edge_row, far], axis=0))
        if step + 1 == STEPS:
            for k in range(3):
                for i in range(rows):
                    stress_out[pl.ds(k, 1), pl.ds(i * LANES, LANES)] = own_stress[k][i : i + 1]
        if step + 1 == STEPS:
            sent = count * halves * (6 + 3 * (STEPS - 1) + 3 * STEPS) + 6 * STEPS + 18
            drain(column_buf.at[pl.ds(0, sent)], send_sem.at[0])
        contact = jnp.zeros((3 * rows, LANES), F32)
        for begin in range(0, group, batch):
            answers = batch - 1 if begin == 0 else batch
            drain(answer_buf.at[step, pl.ds(0, answers), pl.ds(0, 3)], back_sem.at[0, int(begin > 0)])
            for n in range(begin, begin + batch):
                g = arrival[n]
                source = answer_buf if n else back_buf
                halved = split(source[step, g])
                for half in range(halves):
                    match = row_iota == slot_ids[g, pl.ds(half, 1), :]
                    at = pl.ds((n * halves + half) * LANES, LANES)
                    for part in range(2):
                        for k in range(3):
                            row = halved[part][k : k + 1, half * LANES : (half + 1) * LANES]
                            chosen = jnp.where(match, jnp.broadcast_to(row, match.shape), 0.0)
                            pairs[pl.ds((part * 3 + k) * rows, rows), at] = chosen.astype(BF16)
            at = pl.ds(begin * cap, batch * cap)
            summed = nn_dot(pairs[:, at], node_hot[at, :])
            contact += summed[: 3 * rows] + summed[3 * rows :]
        for k in range(3):
            fresh = velocity_rows(k) + pace * (internal[k] + contact[k * rows : (k + 1) * rows])
            vel[pl.ds(k * 2 * rows, rows), :] = fresh
            pos[pl.ds(k * rows, rows), :] = pos[pl.ds(k * rows, rows), :] + TIME_STEP * fresh

    for i in range(rows):
        cols = pl.ds(i * LANES, LANES)
        coords_out[:, cols] = pos[pl.ds(i, 3, stride=rows), :]
        velocity_out[:, cols] = vel[pl.ds(i, 3, stride=2 * rows), :]


def put_out(coords_in, velocity_in, stress_in, coords_out, velocity_out, stress_out, sems):
    pairs = ((coords_in, coords_out), (velocity_in, velocity_out), (stress_in, stress_out))
    copies = [pltpu.make_async_copy(src, dst, sems.at[n]) for n, (src, dst) in enumerate(pairs)]
    for copy in copies:
        copy.start()
    for copy in copies:
        copy.wait()


def per_device(
    sizes, coords, velocity, node_mass, corner_nodes, shape_grad, frame_angles, volume, stress,
    send_nodes, tile_count, tile_nodes, tile_facets, pair_mask,
):
    count = coords.shape[1]
    rows = count // LANES
    group = sizes[1] * sizes[2]
    cap = send_nodes.shape[2]
    tiles = tile_nodes.shape[0]
    vmem = pl.BlockSpec(memory_space=pltpu.VMEM)
    hbm = pl.BlockSpec(memory_space=pltpu.HBM)
    state = jax.ShapeDtypeStruct((3, count), F32)
    halves = cap // LANES
    arrays = (
        coords, velocity, node_mass.reshape(rows, LANES), corner_nodes, shape_grad, frame_angles,
        volume.reshape(rows, LANES), stress, send_nodes, tile_nodes, tile_facets, pair_mask,
    )
    arrays = tuple(pltpu.with_memory_space_constraint(a, pltpu.HBM) for a in arrays)
    dma = pltpu.SemaphoreType.DMA
    finals = pl.pallas_call(
        functools.partial(kernel, sizes),
        out_shape=(state, state, state),
        in_specs=[hbm] * 12 + [pl.BlockSpec(memory_space=pltpu.SMEM)],
        out_specs=(vmem, vmem, vmem),
        scratch_shapes=[pltpu.VMEM(a.shape, a.dtype) for a in arrays] + [
            dma((5,)),
            pltpu.VMEM((3 * rows, LANES), F32),
            pltpu.VMEM((6 * rows, LANES), F32),
            pltpu.VMEM((4 * rows, LANES), jnp.int32),
            pltpu.VMEM((8 * rows, LANES), F32),
            pltpu.VMEM((3 * rows, LANES), F32),
            pltpu.VMEM((2 * rows, LANES), F32),
            pltpu.VMEM((group, halves, LANES), jnp.int32),
            pltpu.VMEM((-(-5 * tiles // 8) * 8, LANES), jnp.int32),
            pltpu.VMEM((rows + 1, LANES, 4 * LANES), BF16),
            pltpu.VMEM((cap, 5 * tiles * LANES), F8),
            pltpu.VMEM((5 * tiles * LANES, cap), F8),
            pltpu.VMEM((group * cap, LANES), F8),
            pltpu.VMEM((4, 16 * (rows + 1), LANES), F32),
            pltpu.VMEM((8 * (rows + 1), LANES), F32),
            pltpu.VMEM((6 * group, 5 * tiles * LANES), BF16),
            pltpu.VMEM((6 * rows, group * cap), BF16),
            pltpu.VMEM((group * cap, LANES), jnp.int32),
            pltpu.VMEM((tiles, LANES, LANES), F32),
            pltpu.VMEM((group, 8, cap), F32),
            pltpu.VMEM((group, 8, cap), F32),
            pltpu.VMEM((STEPS - 1, group, 8, cap), F32),
            pltpu.VMEM((STEPS - 1, group, 8, cap), F32),
            pltpu.VMEM((STEPS, group, 4, cap), F32),
            pltpu.VMEM((STEPS, group, 4, cap), F32),
            pltpu.VMEM((STEPS - 1, 3, LANES), F32),
            pltpu.VMEM((STEPS - 1, 3, LANES), F32),
            pltpu.VMEM((STEPS, 2, 3, LANES), F32),
            pltpu.VMEM((4, LANES), jnp.int32),
            pltpu.VMEM((8, LANES), F32),
            pltpu.VMEM((2, LANES), F32),
            pltpu.VMEM((1, LANES), F32),
            pltpu.VMEM((3, LANES), F32),
            dma((1,)),
            dma((1, 2)),
            dma((1, 2)),
            dma((STEPS + 1,)),
        ],
        compiler_params=pltpu.CompilerParams(
            collective_id=0, has_side_effects=True, vmem_limit_bytes=24 * 1024 * 1024
        ),
    )(*arrays, tile_count)
    return pl.pallas_call(
        put_out,
        out_shape=(state, state, state),
        in_specs=[vmem] * 3,
        out_specs=(hbm, hbm, hbm),
        scratch_shapes=[dma((3,))],
        compiler_params=pltpu.CompilerParams(vmem_limit_bytes=1024 * 1024),
    )(*finals)


def solution(mesh):
    axes = ("len", "wid", "dep")
    flat, wide = P(axes), P(None, axes)
    sizes = tuple(mesh.shape[name] for name in axes)
    return jax.shard_map(
        functools.partial(per_device, sizes),
        mesh=mesh,
        in_specs=(
            wide, wide, flat, wide, wide, wide, flat, wide,
            P(axes, None, None), flat, P(axes, None), P(None, axes, None), P(axes, None, None),
        ),
        out_specs=(wide, wide, wide),
        check_vma=False,
    )
```
